8 devices in a mesh: dp: 8 (over z, y, x, core).
Axes of the slice: x: 2, y: 2, z: 1, core: 2. Of those that a mesh axis runs over, the one named last changes fastest.
Arguments:
- img_emb: bfloat16 [16384, 640], P('dp')
- txt_emb: bfloat16 [16384, 640], P('dp')
- log_temp: float32 [], replicated
- logit_bias: float32 [], replicated
Outputs:
- output 1: float32 [], replicated
- output 2: float32 [16384, 640], P('dp')
- output 3: float32 [16384, 640], P('dp')
- output 4: float32 [], replicated
- output 5: float32 [], replicated
All inputs are finite; a program needn't handle non-finite values.
Results may differ from the reference program's by a relative error of at most 0.001.
Values are sent between devices in bfloat16 or wider.
A program may use at most 1 GiB of HBM per device.

```python
import jax
import jax.numpy as jnp
from jax import lax

EMBED_DIM = 640
ROWS_DEV = 2048
GROUP_SIZE = 8


def setup_inputs(seed: int = 0) -> dict:
    total_rows = ROWS_DEV * GROUP_SIZE
    num_groups = total_rows // 4
    unit_scale = EMBED_DIM ** -0.5
    rand_keys = jax.random.split(jax.random.key(seed), 10)
    shared_dir = jax.random.normal(rand_keys[0], (EMBED_DIM,), jnp.float32) * unit_scale
    centers = jax.random.normal(rand_keys[1], (num_groups, EMBED_DIM), jnp.float32) * unit_scale
    member = jax.random.randint(rand_keys[2], (total_rows,), 0, num_groups)
    own_part = jax.random.normal(rand_keys[3], (total_rows, EMBED_DIM), jnp.float32) * unit_scale
    img_noise = jax.random.normal(rand_keys[4], (total_rows, EMBED_DIM), jnp.float32) * unit_scale
    txt_noise = jax.random.normal(rand_keys[5], (total_rows, EMBED_DIM), jnp.float32) * unit_scale
    common = 0.47 * centers[member] + 0.28 * own_part
    img_scale = jax.random.uniform(rand_keys[6], (total_rows, 1), jnp.float32, minval=20.0, maxval=60.0)
    txt_scale = jax.random.uniform(rand_keys[7], (total_rows, 1), jnp.float32, minval=20.0, maxval=60.0)
    img_emb = (img_scale * (0.35 * shared_dir + common + 0.76 * img_noise)).astype(jnp.bfloat16)
    txt_emb = (txt_scale * (common - 0.35 * shared_dir + 0.76 * txt_noise)).astype(jnp.bfloat16)
    log_temp = jax.random.uniform(rand_keys[8], (), jnp.float32, minval=4.6, maxval=4.8)
    logit_bias = jax.random.uniform(rand_keys[9], (), jnp.float32, minval=-14.0, maxval=-10.0)
    return {"img_emb": img_emb, "txt_emb": txt_emb, "log_temp": log_temp, "logit_bias": logit_bias}


def normalize_rows(emb):
    emb32 = emb.astype(jnp.float32)
    inv_norm = lax.rsqrt(jnp.sum(emb32 * emb32, axis=-1, keepdims=True))
    return emb32 * inv_norm, inv_norm


def project_back(unit_rows, inv_norm, grad_dir):
    radial = jnp.sum(unit_rows * grad_dir, axis=-1, keepdims=True)
    return (grad_dir - unit_rows * radial) * inv_norm


def reference(img_emb, txt_emb, log_temp, logit_bias):
    total_rows = img_emb.shape[0]
    embed_width = img_emb.shape[1]
    block_rows = min(ROWS_DEV, 512)
    num_blocks = total_rows // block_rows
    img_unit, img_inv = normalize_rows(img_emb)
    txt_unit, txt_inv = normalize_rows(txt_emb)
    img_b = img_unit.astype(jnp.bfloat16)
    txt_b = txt_unit.astype(jnp.bfloat16)
    temp_scale = jnp.exp(log_temp)
    col_ids = jnp.arange(total_rows)

    def row_block(acc_state, block_in):
        x_blk, blk_idx = block_in
        loss_sum, weight_sum, weighted_sim, txt_grad = acc_state
        sim_vals = jnp.dot(x_blk, txt_b.T, preferred_element_type=jnp.float32)
        logits = temp_scale * sim_vals + logit_bias
        row_ids = blk_idx * block_rows + jnp.arange(block_rows)
        label_signs = jnp.where(row_ids[:, None] == col_ids[None, :], 1.0, -1.0)
        weights = -label_signs * jax.nn.sigmoid(-label_signs * logits)
        weights_b = weights.astype(jnp.bfloat16)
        new_state = (
            loss_sum + jnp.sum(jax.nn.softplus(-label_signs * logits)),
            weight_sum + jnp.sum(weights),
            weighted_sim + jnp.sum(weights * sim_vals),
            txt_grad + jnp.dot(weights_b.T, x_blk, preferred_element_type=jnp.float32),
        )
        return new_state, jnp.dot(weights_b, txt_b, preferred_element_type=jnp.float32)

    init_state = (
        jnp.zeros((), jnp.float32),
        jnp.zeros((), jnp.float32),
        jnp.zeros((), jnp.float32),
        jnp.zeros((total_rows, embed_width), jnp.float32),
    )
    blocks_in = (img_b.reshape(num_blocks, block_rows, embed_width), jnp.arange(num_blocks))
    final_state, img_parts = lax.scan(row_block, init_state, blocks_in)
    loss_sum, weight_sum, weighted_sim, txt_grad = final_state
    img_dir = temp_scale * img_parts.reshape(total_rows, embed_width)
    txt_dir = temp_scale * txt_grad
    loss_val = loss_sum / total_rows
    grad_img = project_back(img_unit, img_inv, img_dir)
    grad_txt = project_back(txt_unit, txt_inv, txt_dir)
    grad_log_temp = temp_scale * weighted_sim / total_rows
    grad_bias = weight_sum / total_rows
    return (loss_val, grad_img, grad_txt, grad_log_temp, grad_bias)
```

```python
import functools

import jax
import jax.numpy as jnp
from jax import lax
from jax.experimental import pallas as pl
from jax.experimental.pallas import tpu as pltpu
from jax.sharding import PartitionSpec as P

F32, BF16 = jnp.float32, jnp.bfloat16
MESH = pl.DeviceIdType.MESH
LOG2E = 1.4426950408889634
LN2 = 0.6931471805599453
CLAMP = 64.0
TR, TC, LANE = 512, 1024, 128
HALF = TC // 2
HR, HC = 64, 256
SEG = 4

ORDER = [
    (0, 0), (1, 1), (2, 2), (3, 3), (0, 1), (1, 0), (0, 2), (2, 0),
    (4, 0), (4, 1), (0, 4), (1, 4), (2, 4), (3, 4), (4, 4), (4, 2),
    (4, 3), (4, 5), (5, 4), (5, 0), (6, 4), (5, 1), (4, 6), (5, 2),
    (7, 4), (5, 3), (4, 7), (5, 5), (5, 6), (5, 7), (0, 5), (1, 5),
    (2, 5), (3, 5), (6, 5), (7, 5), (6, 0), (6, 1), (6, 2), (6, 3),
    (6, 6), (6, 7), (0, 6), (1, 6), (2, 6), (3, 6), (7, 6), (7, 7),
    (7, 0), (7, 1), (7, 2), (7, 3), (0, 7), (1, 7), (2, 7), (3, 7),
    (0, 3), (3, 0), (1, 2), (2, 1), (1, 3), (3, 1), (2, 3), (3, 2),
]
NT = len(ORDER)
DIAG_TRIPS = 2
FORWARD_TRIP = (3, 6, 9, 11)


def tile_at(trip, parity):
    if isinstance(trip, int):
        return ORDER[2 * trip + parity]
    code = jnp.int32(8 * ORDER[parity][0] + ORDER[parity][1])
    for k in range(1, NT // 2):
        r, g = ORDER[2 * k + parity]
        code = jnp.where(trip == k, 8 * r + g, code)
    return code // 8, code % 8


def last_use(match):
    return max(t for t, rg in enumerate(ORDER) if match(*rg))


def first_use(match):
    return min(t for t, rg in enumerate(ORDER) if match(*rg))


def kernel(scal, x_hbm, xt_hbm, yt_hbm, u_out, v_out, u_in, v_in, vp_in, stats, x_all, xt_all, yt_all, u_all, v_all,
           s0, s1, h0, h1, v_part, loc_sem, img_s, img_r, own_s, own_r, col_s, col_r, fwd_s, fwd_r, u_s, u_r,
           q_s, q_r, v_s, v_r, b_s, b_r, out_sem, free_sem):
    me = lax.axis_index('dp')
    core_nbr, row_nbr, col_nbr = me ^ 1, me ^ 2, me ^ 4
    dim = u_all.shape[0]
    rows = x_hbm.shape[1]
    nblk = rows // LANE
    cblk = HALF // LANE
    kblk = x_hbm.shape[0]

    barrier = pltpu.get_barrier_semaphore()
    for nbr in (core_nbr, row_nbr, col_nbr):
        pl.semaphore_signal(barrier, inc=1, device_id=(nbr,), device_id_type=MESH)

    def remote(src, dst, s, r, k, dev):
        return pltpu.make_async_remote_copy(src_ref=src, dst_ref=dst, send_sem=s.at[k], recv_sem=r.at[k],
                                            device_id=(dev,), device_id_type=MESH)

    def img(k):
        return remote(x_hbm.at[:, pl.ds(k * TR, TR)], x_all.at[:, pl.ds(rows + k * TR, TR)], img_s, img_r, k, row_nbr)

    def own(k):
        return remote(yt_hbm.at[pl.ds(k * cblk, cblk)], yt_all.at[pl.ds(k * 2 * cblk + cblk, cblk)], own_s, own_r, k,
                      core_nbr)

    def col(k):
        return remote(yt_hbm.at[pl.ds(k * cblk, cblk)], yt_all.at[pl.ds((SEG + k) * 2 * cblk, cblk)], col_s, col_r, k,
                      col_nbr)

    def fwd(k):
        return remote(yt_all.at[pl.ds((SEG + k) * 2 * cblk, cblk)], yt_all.at[pl.ds((SEG + k) * 2 * cblk + cblk, cblk)],
                      fwd_s, fwd_r, k, core_nbr)

    def u_send(k):
        return remote(u_all.at[:, pl.ds(rows + k * TR, TR)], u_in.at[:, pl.ds(k * TR, TR)], u_s, u_r, k, row_nbr)

    def q_send(k):
        return remote(v_all.at[:, pl.ds((SEG + k) * TC + HALF, HALF)], v_part.at[k % 2], q_s, q_r, k, core_nbr)

    def v_send(k):
        return remote(v_all.at[:, pl.ds((SEG + k) * TC, HALF)], v_in.at[:, pl.ds(k * HALF, HALF)], v_s, v_r, k, col_nbr)

    def b_send(k):
        return remote(v_all.at[:, pl.ds(k * TC + HALF, HALF)], vp_in.at[:, pl.ds(k * HALF, HALF)], b_s, b_r, k, core_nbr)

    def load(k):
        if k < SEG:
            return pltpu.make_async_copy(yt_hbm.at[pl.ds(k * cblk, cblk)], yt_all.at[pl.ds(k * 2 * cblk, cblk)],
                                         loc_sem.at[k])
        if k == SEG:
            return pltpu.make_async_copy(x_hbm, x_all.at[:, pl.ds(0, rows)], loc_sem.at[k])
        return pltpu.make_async_copy(xt_hbm, xt_all.at[pl.ds(0, nblk)], loc_sem.at[k])

    def store(k):
        if k < SEG:
            return pltpu.make_async_copy(v_all.at[:, pl.ds(k * TC, HALF)], v_out.at[:, pl.ds(k * HALF, HALF)],
                                         out_sem.at[k])
        return pltpu.make_async_copy(u_all.at[:, pl.ds(0, rows)], u_out, out_sem.at[k])

    for k in (SEG, 0, 1, 2, 3, SEG + 1):
        load(k).start()
    pl.semaphore_wait(barrier, 3)
    for k in range(SEG):
        own(k).start()
        img(k).start()
        col(k).start()

    scale2, bias2 = scal[0], scal[1]
    stats[...] = jnp.zeros_like(stats)
    u_all[...] = jnp.zeros_like(u_all)
    v_all[...] = jnp.zeros_like(v_all)
    sim, wgt = (s0, s1), (h0, h1)

    def cat(ref, first, count, rows_at):
        return jnp.concatenate([ref[first + q, rows_at, :] for q in range(count)], axis=1)

    def aligned(start, size):
        return pl.ds(start if isinstance(start, int) else pl.multiple_of(start, size), size)

    every = pl.ds(0, dim)

    def sim_pieces(trip, slot):
        r, g = tile_at(trip, slot)

        def piece(k):
            texts = cat(yt_all, g * 2 * cblk + k * cblk, cblk, every)
            images = cat(x_all, 0, kblk, aligned(r * TR, TR))
            sim[slot][:, k * HALF:(k + 1) * HALF] = jnp.dot(images, texts, preferred_element_type=F32)

        return [functools.partial(piece, k) for k in range(2)]

    def grad_pieces(trip, slot):
        r, g = tile_at(trip, slot)

        def img_piece():
            u_all[:, aligned(r * TR, TR)] += lax.dot_general(
                cat(yt_all, g * 2 * cblk, 2 * cblk, every), cat(wgt[slot], 0, 2 * cblk, pl.ds(0, TR)),
                (((1,), (1,)), ((), ())), preferred_element_type=F32)

        def txt_piece(k):
            v_all[:, aligned(g * TC + k * HALF, HALF)] += jnp.dot(
                cat(xt_all, r * (TR // LANE), TR // LANE, every), cat(wgt[slot], k * cblk, cblk, pl.ds(0, TR)),
                preferred_element_type=F32)

        return [img_piece] + [functools.partial(txt_piece, k) for k in range(2)]

    def weight_pieces(trip, slot, count, diag):
        blocks = [(r, c) for r in range(0, TR, HR) for c in range(0, TC, HC)]
        per = -(-len(blocks) // count)
        sums = [None] * 4
        if diag:
            tr, tg = tile_at(trip, slot)
            offset = jnp.where(tr == tg, 0, 4 * TC)
            lag = lax.broadcasted_iota(jnp.int32, (HR, HC), 1) - lax.broadcasted_iota(jnp.int32, (HR, HC), 0)

        def fold(q):
            return jnp.sum(q.reshape(HR // 8, 8, HC), axis=0)

        def piece(k):
            for r, c in blocks[k * per:(k + 1) * per]:
                on_diag = diag and c < HALF and r < c + HC and c < r + HR
                s = sim[slot][r:r + HR, c:c + HC]
                logit2 = s * scale2 + bias2
                if on_diag:
                    same = lag == r - c + offset
                    logit2 = jnp.where(same, -logit2, logit2)
                clamped = jnp.minimum(logit2, CLAMP)
                e = jnp.exp2(clamped)
                v = 1.0 + e
                inv = 1.0 / v
                h = e * inv
                kept = (v - 1.0) * inv
                if on_diag:
                    signed = jnp.where(same, -h, h)
                    kept = kept - h + signed
                    h = signed
                hb = h.astype(BF16)
                for cc in range(0, HC, LANE):
                    wgt[slot][(c + cc) // LANE, r:r + HR, :] = hb[:, cc:cc + LANE]
                for q, part in enumerate((jnp.log2(v) + (logit2 - clamped), kept, h, h * s)):
                    part = fold(part)
                    sums[q] = part if sums[q] is None else sums[q] + part
            if k == count - 1:
                for q in range(4):
                    stats[q] += sums[q]

        return [functools.partial(piece, k) for k in range(count)]

    def step(trip, slot, diag):
        mxu = sim_pieces(trip + 1, slot) + grad_pieces(trip, slot)
        vpu = weight_pieces(trip + slot, 1 - slot, len(mxu), diag)
        for a, b in zip(mxu, vpu):
            a()
            b()

    def take_img(k):
        img(k).wait_recv()
        for kb in range(kblk):
            block = x_all[kb, rows + k * TR:rows + (k + 1) * TR, :].astype(F32).T.astype(BF16)
            for q in range(TR // LANE):
                xt_all[nblk + k * (TR // LANE) + q, kb * LANE:(kb + 1) * LANE, :] = block[:, q * LANE:(q + 1) * LANE]

    def pass_on(k):
        col(k).wait_recv()
        fwd(k).start()

    def add_part(k):
        q_send(k).wait_recv()
        v_all[:, (SEG + k) * TC:(SEG + k) * TC + HALF] += v_part[k % 2]
        if k + 2 < SEG:
            pl.semaphore_signal(free_sem, inc=1, device_id=(core_nbr,), device_id_type=MESH)

    def send_part(k):
        if k >= 2:
            pl.semaphore_wait(free_sem, 1)
        q_send(k).start()

    events = {}

    def at(trip, fn, k):
        events.setdefault(trip, []).append(functools.partial(fn, k))

    for k in range(SEG):
        if k >= 2:
            at((first_use(lambda r, g: g == k) - 2) // 2, lambda k: (load(k).wait(), own(k).wait_recv()), k)
        at(FORWARD_TRIP[k], pass_on, k)
        use = (first_use(lambda r, g: g == SEG + k) - 2) // 2
        assert use > FORWARD_TRIP[k]
        at(use, lambda k: fwd(k).wait_recv(), k)
        at((first_use(lambda r, g: r == SEG + k) - 2) // 2, take_img, k)
        at(last_use(lambda r, g: r == SEG + k) // 2 + 1, lambda k: u_send(k).start(), k)
        done = last_use(lambda r, g: g == SEG + k) // 2 + 1
        at(done, send_part, k)
        at(done + 1, add_part, k)
        at(done + 2, lambda k: v_send(k).start(), k)

    def trips(first, last, diag):
        def body(p, carry):
            for trip in range(first, last):
                if trip in events:
                    @pl.when(p == trip)
                    def _():
                        for fn in events[trip]:
                            fn()
            step(p, 0, diag)
            step(p, 1, diag)
            return carry
        lax.fori_loop(first, last, body, 0)

    load(SEG).wait()
    for k in range(2):
        load(k).wait()
        own(k).wait_recv()
        for piece in sim_pieces(0, k):
            piece()
        if k == 0:
            for piece in weight_pieces(0, 0, 1, True):
                piece()
    load(SEG + 1).wait()
    last = NT // 2 - 1
    trips(0, DIAG_TRIPS, True)
    trips(DIAG_TRIPS, last, False)
    assert max(events) < last
    for piece in grad_pieces(last, 0) + weight_pieces(last, 1, 1, False) + grad_pieces(last, 1):
        piece()
    for k in range(SEG):
        b_send(k).start()
    for k in range(SEG + 1):
        store(k).start()
    for k in range(SEG + 1):
        store(k).wait()
    for k in range(SEG):
        img(k).wait_send()
        own(k).wait_send()
        col(k).wait_send()
        fwd(k).wait_send()
        q_send(k).wait_send()
        for copy in (u_send(k), v_send(k), b_send(k)):
            copy.wait()


def normalize_rows(emb):
    emb32 = emb.astype(F32)
    inv_norm = lax.rsqrt(jnp.sum(emb32 * emb32, axis=-1, keepdims=True))
    return emb32 * inv_norm, inv_norm


def project_back(unit_rows, inv_norm, grad_dir):
    radial = jnp.sum(unit_rows * grad_dir, axis=-1, keepdims=True)
    return (grad_dir - unit_rows * radial) * inv_norm


def lane_blocks(mat):
    return mat.reshape(mat.shape[0], mat.shape[1] // LANE, LANE).transpose(1, 0, 2)


def solution(mesh):
    group_size = mesh.shape['dp']

    def local_fn(img_emb, txt_emb, log_temp, logit_bias):
        rows, dim = img_emb.shape
        total_rows = rows * group_size
        img_unit, img_inv = normalize_rows(img_emb)
        txt_unit, txt_inv = normalize_rows(txt_emb)
        img_b = img_unit.astype(BF16)
        txt_b = txt_unit.astype(BF16)
        temp_scale = jnp.exp(log_temp)
        scal = jnp.stack([temp_scale * LOG2E, logit_bias * LOG2E])
        nblk, kblk = rows // LANE, dim // LANE
        half_out = jax.ShapeDtypeStruct((dim, rows), F32)
        any_spec = pl.BlockSpec(memory_space=pl.ANY)
        dma = pltpu.SemaphoreType.DMA
        u_own, v_own, u_in, v_in, vp_in, stats = pl.pallas_call(
            kernel,
            out_shape=[half_out] * 5 + [jax.ShapeDtypeStruct((4, 8, HC), F32)],
            in_specs=[pl.BlockSpec(memory_space=pltpu.SMEM)] + [any_spec] * 3,
            out_specs=[any_spec] * 5 + [pl.BlockSpec(memory_space=pltpu.VMEM)],
            scratch_shapes=[
                pltpu.VMEM((kblk, 2 * rows, LANE), BF16),
                pltpu.VMEM((2 * nblk, dim, LANE), BF16),
                pltpu.VMEM((4 * nblk, dim, LANE), BF16),
                pltpu.VMEM((dim, 2 * rows), F32),
                pltpu.VMEM((dim, 4 * rows), F32),
                pltpu.VMEM((TR, TC), F32),
                pltpu.VMEM((TR, TC), F32),
                pltpu.VMEM((TC // LANE, TR, LANE), BF16),
                pltpu.VMEM((TC // LANE, TR, LANE), BF16),
                pltpu.VMEM((2, dim, HALF), F32),
                dma((SEG + 2,)),
            ] + [dma((SEG,))] * 16 + [dma((SEG + 1,)), pltpu.SemaphoreType.REGULAR],
            compiler_params=pltpu.CompilerParams(
                collective_id=0, has_side_effects=True, vmem_limit_bytes=67043328),
        )(scal, lane_blocks(img_b), lane_blocks(img_b.T), lane_blocks(txt_b.T))
        sums = lax.psum(jnp.sum(stats, axis=(1, 2)), 'dp') / total_rows
        loss = LN2 * sums[0] + (sums[2] - sums[1])
        grad_img = project_back(img_unit, img_inv, temp_scale * (u_own + u_in).T)
        grad_txt = project_back(txt_unit, txt_inv, temp_scale * ((v_own + vp_in) + v_in).T)
        return loss, grad_img, grad_txt, temp_scale * sums[3], sums[2]

    return jax.shard_map(
        local_fn,
        mesh=mesh,
        in_specs=(P('dp', None), P('dp', None), P(), P()),
        out_specs=(P(), P('dp', None), P('dp', None), P(), P()),
        check_vma=False,
    )
```

```python
import functools

import jax
import jax.numpy as jnp
from jax import lax
from jax.experimental import pallas as pl
from jax.experimental.pallas import tpu as pltpu
from jax.sharding import PartitionSpec as P

F32, BF16 = jnp.float32, jnp.bfloat16
MESH = pl.DeviceIdType.MESH
LOG2E = 1.4426950408889634
LN2 = 0.6931471805599453
CLAMP = 64.0
TR, TC, LANE = 512, 1024, 128
HALF = TC // 2
HR, HC = 64, 256
SEG = 4

ORDER = [
    (0, 0), (1, 1), (2, 2), (3, 3), (0, 1), (1, 0), (0, 2), (2, 0),
    (4, 0), (4, 1), (0, 4), (1, 4), (2, 4), (3, 4), (4, 4), (4, 2),
    (4, 3), (4, 5), (5, 4), (5, 0), (6, 4), (5, 1), (4, 6), (5, 2),
    (7, 4), (5, 3), (4, 7), (5, 5), (5, 6), (5, 7), (0, 5), (1, 5),
    (2, 5), (3, 5), (6, 5), (7, 5), (6, 0), (6, 1), (6, 2), (6, 3),
    (6, 6), (6, 7), (0, 6), (1, 6), (2, 6), (3, 6), (7, 6), (7, 7),
    (7, 0), (7, 1), (7, 2), (7, 3), (0, 7), (1, 7), (2, 7), (3, 7),
    (0, 3), (3, 0), (1, 2), (2, 1), (1, 3), (3, 1), (2, 3), (3, 2),
]
NT = len(ORDER)
DIAG_TRIPS = 2
FORWARD_TRIP = (3, 6, 9, 11)


def tile_at(trip, parity):
    if isinstance(trip, int):
        return ORDER[2 * trip + parity]
    code = jnp.int32(8 * ORDER[parity][0] + ORDER[parity][1])
    for k in range(1, NT // 2):
        r, g = ORDER[2 * k + parity]
        code = jnp.where(trip == k, 8 * r + g, code)
    return code // 8, code % 8


def last_use(match):
    return max(t for t, rg in enumerate(ORDER) if match(*rg))


def first_use(match):
    return min(t for t, rg in enumerate(ORDER) if match(*rg))


def kernel(scal, img_hbm, txt_hbm, u_out, v_out, u_in, v_in, vp_in, sums_out, stats, st_buf, st_in, x_all, xt_all, yt_all, u_all, v_all,
           s0, s1, h0, h1, v_part, x_sem, y_sem, img_s, img_r, own_s, own_r, col_s, col_r, fwd_s, fwd_r, u_s, u_r,
           q_s, q_r, v_s, v_r, b_s, b_r, out_sem, st_s, st_r, free_sem):
    me = lax.axis_index('dp')
    core_nbr, row_nbr, col_nbr = me ^ 1, me ^ 2, me ^ 4
    dim = u_all.shape[0]
    rows = img_hbm.shape[0]
    nblk = rows // LANE
    cblk = HALF // LANE
    kblk = dim // LANE

    barrier = pltpu.get_barrier_semaphore()
    for nbr in (core_nbr, row_nbr, col_nbr):
        pl.semaphore_signal(barrier, inc=1, device_id=(nbr,), device_id_type=MESH)

    def remote(src, dst, s, r, k, dev):
        return pltpu.make_async_remote_copy(src_ref=src, dst_ref=dst, send_sem=s.at[k], recv_sem=r.at[k],
                                            device_id=(dev,), device_id_type=MESH)

    def img(k):
        return remote(x_all.at[:, pl.ds(k * TR, TR)], x_all.at[:, pl.ds(rows + k * TR, TR)], img_s, img_r, k, row_nbr)

    def own(k):
        return remote(yt_all.at[pl.ds(k * 2 * cblk, cblk)], yt_all.at[pl.ds(k * 2 * cblk + cblk, cblk)], own_s, own_r, k,
                      core_nbr)

    def col(k):
        return remote(yt_all.at[pl.ds(k * 2 * cblk, cblk)], yt_all.at[pl.ds((SEG + k) * 2 * cblk, cblk)], col_s, col_r, k,
                      col_nbr)

    def fwd(k):
        return remote(yt_all.at[pl.ds((SEG + k) * 2 * cblk, cblk)], yt_all.at[pl.ds((SEG + k) * 2 * cblk + cblk, cblk)],
                      fwd_s, fwd_r, k, core_nbr)

    def u_send(k):
        return remote(u_all.at[:, pl.ds(rows + k * TR, TR)], u_in.at[:, pl.ds(k * TR, TR)], u_s, u_r, k, row_nbr)

    def q_send(k):
        return remote(v_all.at[:, pl.ds((SEG + k) * TC + HALF, HALF)], v_part.at[k % 2], q_s, q_r, k, core_nbr)

    def v_send(k):
        return remote(v_all.at[:, pl.ds((SEG + k) * TC, HALF)], v_in.at[:, pl.ds(k * HALF, HALF)], v_s, v_r, k, col_nbr)

    def b_send(k):
        return remote(v_all.at[:, pl.ds(k * TC + HALF, HALF)], vp_in.at[:, pl.ds(k * HALF, HALF)], b_s, b_r, k, core_nbr)

    def load_img(kb):
        return pltpu.make_async_copy(img_hbm.at[:, pl.ds(kb * LANE, LANE)], x_all.at[kb, pl.ds(0, rows)], x_sem.at[kb])

    def load_txt(k, kb):
        return pltpu.make_async_copy(txt_hbm.at[pl.ds(k * TR, TR), pl.ds(kb * LANE, LANE)],
                                     wgt[k % 2].at[kb], y_sem.at[k * kblk + kb])

    def swap(k, value):
        nbr = (core_nbr, row_nbr, col_nbr)[k]
        st_buf[k] = value
        copy = remote(st_buf.at[k], st_in.at[k], st_s, st_r, k, nbr)
        copy.start()
        copy.wait()
        return st_buf[k] + st_in[k]

    def store(k):
        if k < SEG:
            return pltpu.make_async_copy(v_all.at[:, pl.ds(k * TC, HALF)], v_out.at[:, pl.ds(k * HALF, HALF)],
                                         out_sem.at[k])
        return pltpu.make_async_copy(u_all.at[:, pl.ds(0, rows)], u_out, out_sem.at[k])

    sim, wgt = (s0, s1), (h0, h1)
    for kb in range(kblk):
        load_txt(0, kb).start()
    for kb in range(kblk):
        load_img(kb).start()
    for kb in range(kblk):
        load_txt(1, kb).start()

    def unit(blocks):
        wide = [block.astype(F32) for block in blocks]
        norm2 = jnp.sum(functools.reduce(jnp.add, [w * w for w in wide]), axis=-1, keepdims=True)
        inv_norm = lax.rsqrt(norm2)
        return [(w * inv_norm).astype(BF16) for w in wide]

    def put_transposed(ref, first, kb, block):
        flipped = block.T
        for q in range(TR // LANE):
            ref[first + q, kb * LANE:(kb + 1) * LANE, :] = flipped[:, q * LANE:(q + 1) * LANE]

    for k in range(SEG):
        for kb in range(kblk):
            load_txt(k, kb).wait()
        for kb, block in enumerate(unit([wgt[k % 2][kb] for kb in range(kblk)])):
            put_transposed(yt_all, k * 2 * cblk, kb, block)
        if k == 0:
            for kb in range(kblk):
                load_img(kb).wait()
        if k + 2 < SEG:
            for kb in range(kblk):
                load_txt(k + 2, kb).start()
        at_rows = slice(k * TR, (k + 1) * TR)
        for kb, block in enumerate(unit([x_all[kb, at_rows, :] for kb in range(kblk)])):
            x_all[kb, at_rows, :] = block
            put_transposed(xt_all, k * (TR // LANE), kb, block)
        if k == 0:
            pl.semaphore_wait(barrier, 3)
        col(k).start()
        img(k).start()
        own(k).start()

    scale2, bias2 = scal[0], scal[1]
    stats[...] = jnp.zeros_like(stats)
    u_all[...] = jnp.zeros_like(u_all)
    v_all[...] = jnp.zeros_like(v_all)

    def cat(ref, first, count, rows_at):
        return jnp.concatenate([ref[first + q, rows_at, :] for q in range(count)], axis=1)

    def aligned(start, size):
        return pl.ds(start if isinstance(start, int) else pl.multiple_of(start, size), size)

    every = pl.ds(0, dim)

    def sim_pieces(trip, slot):
        r, g = tile_at(trip, slot)

        def piece(k):
            texts = cat(yt_all, g * 2 * cblk + k * cblk, cblk, every)
            images = cat(x_all, 0, kblk, aligned(r * TR, TR))
            sim[slot][:, k * HALF:(k + 1) * HALF] = jnp.dot(images, texts, preferred_element_type=F32)

        return [functools.partial(piece, k) for k in range(2)]

    def grad_pieces(trip, slot):
        r, g = tile_at(trip, slot)

        def img_piece():
            u_all[:, aligned(r * TR, TR)] += lax.dot_general(
                cat(yt_all, g * 2 * cblk, 2 * cblk, every), cat(wgt[slot], 0, 2 * cblk, pl.ds(0, TR)),
                (((1,), (1,)), ((), ())), preferred_element_type=F32)

        def txt_piece(k):
            v_all[:, aligned(g * TC + k * HALF, HALF)] += jnp.dot(
                cat(xt_all, r * (TR // LANE), TR // LANE, every), cat(wgt[slot], k * cblk, cblk, pl.ds(0, TR)),
                preferred_element_type=F32)

        return [img_piece] + [functools.partial(txt_piece, k) for k in range(2)]

    def weight_pieces(trip, slot, count, diag):
        blocks = [(r, c) for r in range(0, TR, HR) for c in range(0, TC, HC)]
        per = -(-len(blocks) // count)
        sums = [None] * 4
        if diag:
            tr, tg = tile_at(trip, slot)
            offset = jnp.where(tr == tg, 0, 4 * TC)
            lag = lax.broadcasted_iota(jnp.int32, (HR, HC), 1) - lax.broadcasted_iota(jnp.int32, (HR, HC), 0)

        def fold(q):
            return jnp.sum(q.reshape(HR // 8, 8, HC), axis=0)

        def piece(k):
            for r, c in blocks[k * per:(k + 1) * per]:
                on_diag = diag and c < HALF and r < c + HC and c < r + HR
                s = sim[slot][r:r + HR, c:c + HC]
                logit2 = s * scale2 + bias2
                if on_diag:
                    same = lag == r - c + offset
                    logit2 = jnp.where(same, -logit2, logit2)
                clamped = jnp.minimum(logit2, CLAMP)
                e = jnp.exp2(clamped)
                v = 1.0 + e
                inv = 1.0 / v
                h = e * inv
                kept = (v - 1.0) * inv
                if on_diag:
                    signed = jnp.where(same, -h, h)
                    kept = kept - h + signed
                    h = signed
                hb = h.astype(BF16)
                for cc in range(0, HC, LANE):
                    wgt[slot][(c + cc) // LANE, r:r + HR, :] = hb[:, cc:cc + LANE]
                for q, part in enumerate((jnp.log2(v) + (logit2 - clamped), kept, h, h * s)):
                    part = fold(part)
                    sums[q] = part if sums[q] is None else sums[q] + part
            if k == count - 1:
                for q in range(4):
                    stats[q] += sums[q]

        return [functools.partial(piece, k) for k in range(count)]

    def step(trip, slot, diag):
        mxu = sim_pieces(trip + 1, slot) + grad_pieces(trip, slot)
        vpu = weight_pieces(trip + slot, 1 - slot, len(mxu), diag)
        for a, b in zip(mxu, vpu):
            a()
            b()

    def take_img(k):
        img(k).wait_recv()
        for kb in range(kblk):
            put_transposed(xt_all, nblk + k * (TR // LANE), kb, x_all[kb, rows + k * TR:rows + (k + 1) * TR, :])

    def pass_on(k):
        col(k).wait_recv()
        fwd(k).start()

    def add_part(k):
        q_send(k).wait_recv()
        v_all[:, (SEG + k) * TC:(SEG + k) * TC + HALF] += v_part[k % 2]
        if k + 2 < SEG:
            pl.semaphore_signal(free_sem, inc=1, device_id=(core_nbr,), device_id_type=MESH)

    def send_part(k):
        if k >= 2:
            pl.semaphore_wait(free_sem, 1)
        q_send(k).start()

    events = {}

    def at(trip, fn, k):
        events.setdefault(trip, []).append(functools.partial(fn, k))

    for k in range(SEG):
        if k >= 2:
            at((first_use(lambda r, g: g == k) - 2) // 2, lambda k: own(k).wait_recv(), k)
        at(FORWARD_TRIP[k], pass_on, k)
        use = (first_use(lambda r, g: g == SEG + k) - 2) // 2
        assert use > FORWARD_TRIP[k]
        at(use, lambda k: fwd(k).wait_recv(), k)
        at((first_use(lambda r, g: r == SEG + k) - 2) // 2, take_img, k)
        at(last_use(lambda r, g: r == SEG + k) // 2 + 1, lambda k: u_send(k).start(), k)
        done = last_use(lambda r, g: g == SEG + k) // 2 + 1
        at(done, send_part, k)
        at(done + 1, add_part, k)
        at(done + 2, lambda k: v_send(k).start(), k)

    def trips(first, last, diag):
        def body(p, carry):
            for trip in range(first, last):
                if trip in events:
                    @pl.when(p == trip)
                    def _():
                        for fn in events[trip]:
                            fn()
            step(p, 0, diag)
            step(p, 1, diag)
            return carry
        lax.fori_loop(first, last, body, 0)

    for k in range(2):
        own(k).wait_recv()
        for piece in sim_pieces(0, k):
            piece()
        if k == 0:
            for piece in weight_pieces(0, 0, 1, True):
                piece()
    last = NT // 2 - 1
    trips(0, DIAG_TRIPS, True)
    trips(DIAG_TRIPS, last, False)
    assert max(events) < last
    for piece in grad_pieces(last, 0) + weight_pieces(last, 1, 1, False) + grad_pieces(last, 1):
        piece()
    for k in range(SEG):
        b_send(k).start()
    for k in range(SEG + 1):
        store(k).start()
    total = stats[:, :, :LANE]
    for c in range(LANE, HC, LANE):
        total += stats[:, :, c:c + LANE]
    for k in range(3):
        total = swap(k, total)
    for q in range(4):
        sums_out[q] = jnp.sum(total[q])
    for k in range(SEG + 1):
        store(k).wait()
    for k in range(SEG):
        img(k).wait_send()
        own(k).wait_send()
        col(k).wait_send()
        fwd(k).wait_send()
        q_send(k).wait_send()
        for copy in (u_send(k), v_send(k), b_send(k)):
            copy.wait()


def finish(temp, img, txt, u_own, u_in, v_own, vp_in, v_in, img_out, txt_out):
    def project(emb, total, out):
        emb32 = emb[...].astype(F32)
        inv_norm = lax.rsqrt(jnp.sum(emb32 * emb32, axis=-1, keepdims=True))
        unit_rows = emb32 * inv_norm
        grad_dir = (total * temp[0]).T
        radial = jnp.sum(unit_rows * grad_dir, axis=-1, keepdims=True)
        out[...] = (grad_dir - unit_rows * radial) * inv_norm

    project(img, u_own[...] + u_in[...], img_out)
    project(txt, (v_own[...] + vp_in[...]) + v_in[...], txt_out)


def solution(mesh):
    group_size = mesh.shape['dp']

    def local_fn(img_emb, txt_emb, log_temp, logit_bias):
        rows, dim = img_emb.shape
        total_rows = rows * group_size
        temp_scale = jnp.exp(log_temp)
        scal = jnp.stack([temp_scale * LOG2E, logit_bias * LOG2E])
        nblk, kblk = rows // LANE, dim // LANE
        half_out = jax.ShapeDtypeStruct((dim, rows), F32)
        any_spec = pl.BlockSpec(memory_space=pl.ANY)
        smem_spec = pl.BlockSpec(memory_space=pltpu.SMEM)
        dma = pltpu.SemaphoreType.DMA
        u_own, v_own, u_in, v_in, vp_in, sums = pl.pallas_call(
            kernel,
            out_shape=[half_out] * 5 + [jax.ShapeDtypeStruct((4,), F32)],
            in_specs=[smem_spec] + [any_spec] * 2,
            out_specs=[any_spec] * 5 + [smem_spec],
            scratch_shapes=[
                pltpu.VMEM((4, 8, HC), F32),
                pltpu.VMEM((3, 4, 8, LANE), F32),
                pltpu.VMEM((3, 4, 8, LANE), F32),
                pltpu.VMEM((kblk, 2 * rows, LANE), BF16),
                pltpu.VMEM((2 * nblk, dim, LANE), BF16),
                pltpu.VMEM((4 * nblk, dim, LANE), BF16),
                pltpu.VMEM((dim, 2 * rows), F32),
                pltpu.VMEM((dim, 4 * rows), F32),
                pltpu.VMEM((TR, TC), F32),
                pltpu.VMEM((TR, TC), F32),
                pltpu.VMEM((TC // LANE, TR, LANE), BF16),
                pltpu.VMEM((TC // LANE, TR, LANE), BF16),
                pltpu.VMEM((2, dim, HALF), F32),
                dma((kblk,)),
                dma((SEG * kblk,)),
            ] + [dma((SEG,))] * 16 + [dma((SEG + 1,)), dma((3,)), dma((3,)), pltpu.SemaphoreType.REGULAR],
            compiler_params=pltpu.CompilerParams(
                collective_id=0, has_side_effects=True, vmem_limit_bytes=67043328),
        )(scal, img_emb, txt_emb)
        sums = sums / total_rows
        loss = LN2 * sums[0] + (sums[2] - sums[1])
        step_rows = 256
        emb_spec = pl.BlockSpec((step_rows, dim), lambda i: (i, 0))
        col_spec = pl.BlockSpec((dim, step_rows), lambda i: (0, i))
        grad_img, grad_txt = pl.pallas_call(
            finish,
            grid=(rows // step_rows,),
            out_shape=[jax.ShapeDtypeStruct((rows, dim), F32)] * 2,
            in_specs=[smem_spec] + [emb_spec] * 2 + [col_spec] * 5,
            out_specs=[emb_spec] * 2,
        )(temp_scale[None], img_emb, txt_emb, u_own, u_in, v_own, vp_in, v_in)
        return loss, grad_img, grad_txt, temp_scale * sums[3], sums[2]

    return jax.shard_map(
        local_fn,
        mesh=mesh,
        in_specs=(P('dp', None), P('dp', None), P(), P()),
        out_specs=(P(), P('dp', None), P('dp', None), P(), P()),
        check_vma=False,
    )
```

```python
import functools

import jax
import jax.numpy as jnp
from jax import lax
from jax.experimental import pallas as pl
from jax.experimental.pallas import tpu as pltpu
from jax.sharding import PartitionSpec as P

F32, BF16 = jnp.float32, jnp.bfloat16
MESH = pl.DeviceIdType.MESH
LOG2E = 1.4426950408889634
LN2 = 0.6931471805599453
CLAMP = 64.0
TR, TC, LANE = 512, 1024, 128
HALF = TC // 2
HR, HC = 64, 256
SEG = 4

ORDER = [
    (0, 0), (1, 1), (2, 2), (3, 3), (0, 1), (1, 0), (4, 0), (4, 1),
    (4, 2), (4, 3), (0, 4), (1, 4), (2, 4), (3, 4), (4, 4), (5, 4),
    (4, 5), (6, 4), (4, 6), (5, 0), (5, 1), (5, 5), (7, 4), (5, 6),
    (4, 7), (5, 2), (5, 3), (5, 7), (0, 5), (1, 5), (2, 5), (3, 5),
    (6, 5), (7, 5), (6, 0), (6, 1), (6, 2), (6, 3), (6, 6), (6, 7),
    (0, 6), (1, 6), (2, 6), (3, 6), (7, 6), (7, 7), (7, 0), (7, 1),
    (7, 2), (7, 3), (0, 7), (1, 7), (2, 7), (3, 7), (2, 0), (3, 0),
    (2, 1), (3, 1), (0, 2), (1, 2), (3, 2), (0, 3), (1, 3), (2, 3),
]
assert len(set(ORDER)) == 64
NT = len(ORDER)
DIAG_TRIPS = 2
FORWARD_TRIP = (2, 6, 7, 10)


def code_at(trip, parity):
    codes = [8 * r + g for r, g in ORDER[parity::2]]
    if isinstance(trip, int):
        return codes[trip]
    code = jnp.int32(codes[0])
    for k, value in enumerate(codes[1:], 1):
        code = jnp.where(trip == k, value, code)
    return code


def last_use(match):
    return max(t for t, rg in enumerate(ORDER) if match(*rg))


def first_use(match):
    return min(t for t, rg in enumerate(ORDER) if match(*rg))


def kernel(scal, img_hbm, txt_hbm, u_out, v_out, u_in, v_in, vp_in, sums_out, stats, st_buf, st_in, x_all, xt_all, yt_all, u_all, v_all,
           s0, s1, h0, h1, v_part, x_sem, y_sem, img_s, img_r, own_s, own_r, col_s, col_r, fwd_s, fwd_r, u_s, u_r,
           q_s, q_r, v_s, v_r, b_s, b_r, out_sem, st_s, st_r, in_sem, free_sem):
    me = lax.axis_index('dp')
    core_nbr, row_nbr, col_nbr = me ^ 1, me ^ 2, me ^ 4
    dim = u_all.shape[0]
    rows = img_hbm.shape[0]
    nblk = rows // LANE
    cblk = HALF // LANE
    kblk = dim // LANE

    barrier = pltpu.get_barrier_semaphore()
    for nbr in (core_nbr, row_nbr, col_nbr):
        pl.semaphore_signal(barrier, inc=1, device_id=(nbr,), device_id_type=MESH)

    def remote(src, dst, s, r, k, dev):
        return pltpu.make_async_remote_copy(src_ref=src, dst_ref=dst, send_sem=s.at[k], recv_sem=r.at[k],
                                            device_id=(dev,), device_id_type=MESH)

    def img(k):
        return remote(x_all.at[:, pl.ds(k * TR, TR)], x_all.at[:, pl.ds(rows + k * TR, TR)], img_s, img_r, k, row_nbr)

    def own(k):
        return remote(yt_all.at[pl.ds(k * 2 * cblk, cblk)], yt_all.at[pl.ds(k * 2 * cblk + cblk, cblk)], own_s, own_r, k,
                      core_nbr)

    def col(k):
        return remote(yt_all.at[pl.ds(k * 2 * cblk, cblk)], yt_all.at[pl.ds((SEG + k) * 2 * cblk, cblk)], col_s, col_r, k,
                      col_nbr)

    def fwd(k):
        return remote(yt_all.at[pl.ds((SEG + k) * 2 * cblk, cblk)], yt_all.at[pl.ds((SEG + k) * 2 * cblk + cblk, cblk)],
                      fwd_s, fwd_r, k, core_nbr)

    def u_send(k):
        return remote(u_all.at[:, pl.ds(rows + k * TR, TR)], u_in.at[:, pl.ds(k * TR, TR)], u_s, u_r, k, row_nbr)

    def q_send(k):
        return remote(v_all.at[:, pl.ds((SEG + k) * TC + HALF, HALF)], v_part.at[k % 2], q_s, q_r, k, core_nbr)

    def v_send(k):
        return remote(v_all.at[:, pl.ds((SEG + k) * TC, HALF)], v_in.at[:, pl.ds(k * HALF, HALF)], v_s, v_r, k, col_nbr)

    def b_send(k):
        return remote(v_all.at[:, pl.ds(k * TC + HALF, HALF)], vp_in.at[:, pl.ds(k * HALF, HALF)], b_s, b_r, k, core_nbr)

    def load_img(kb):
        return pltpu.make_async_copy(img_hbm.at[:, pl.ds(kb * LANE, LANE)], x_all.at[kb, pl.ds(0, rows)], x_sem.at[kb])

    def load_txt(k, kb):
        return pltpu.make_async_copy(txt_hbm.at[pl.ds(k * TR, TR), pl.ds(kb * LANE, LANE)],
                                     wgt[k % 2].at[kb], y_sem.at[k * kblk + kb])

    def swap(k, value):
        nbr = (core_nbr, row_nbr, col_nbr)[k]
        st_buf[k] = value
        copy = remote(st_buf.at[k], st_in.at[k], st_s, st_r, k, nbr)
        copy.start()
        copy.wait()
        return st_buf[k] + st_in[k]

    def load_img(kb):
        return pltpu.make_async_copy(img_hbm.at[:, pl.ds(kb * LANE, LANE)], x_all.at[kb, pl.ds(0, rows)], x_sem.at[kb])

    def load_txt(k, kb):
        return pltpu.make_async_copy(txt_hbm.at[pl.ds(k * TR, TR), pl.ds(kb * LANE, LANE)],
                                     wgt[k % 2].at[kb], y_sem.at[k * kblk + kb])

    def swap(k, value):
        nbr = (core_nbr, row_nbr, col_nbr)[k]
        st_buf[k] = value
        copy = remote(st_buf.at[k], st_in.at[k], st_s, st_r, k, nbr)
        copy.start()
        copy.wait()
        return st_buf[k] + st_in[k]

    def store(k):
        if k < SEG:
            return pltpu.make_async_copy(v_all.at[:, pl.ds(k * TC, HALF)], v_out.at[:, pl.ds(k * HALF, HALF)],
                                         out_sem.at[k])
        return pltpu.make_async_copy(u_all.at[:, pl.ds(0, rows)], u_out, out_sem.at[k])

    sim, wgt = (s0, s1), (h0, h1)
    for kb in range(kblk):
        load_txt(0, kb).start()
    for kb in range(kblk):
        load_img(kb).start()
    for kb in range(kblk):
        load_txt(1, kb).start()

    u_all[...] = jnp.zeros_like(u_all)

    def unit(blocks):
        wide = [block.astype(F32) for block in blocks]
        norm2 = jnp.sum(functools.reduce(jnp.add, [w * w for w in wide]), axis=-1, keepdims=True)
        inv_norm = lax.rsqrt(norm2)
        return [(w * inv_norm).astype(BF16) for w in wide]

    def put_transposed(ref, first, kb, block):
        flipped = block.T
        for q in range(TR // LANE):
            ref[first + q, kb * LANE:(kb + 1) * LANE, :] = flipped[:, q * LANE:(q + 1) * LANE]

    for k in range(SEG):
        for kb in range(kblk):
            load_txt(k, kb).wait()
        for kb, block in enumerate(unit([wgt[k % 2][kb] for kb in range(kblk)])):
            put_transposed(yt_all, k * 2 * cblk, kb, block)
        if k == 0:
            for kb in range(kblk):
                load_img(kb).wait()
        if k + 2 < SEG:
            for kb in range(kblk):
                load_txt(k + 2, kb).start()
        at_rows = slice(k * TR, (k + 1) * TR)
        for kb, block in enumerate(unit([x_all[kb, at_rows, :] for kb in range(kblk)])):
            x_all[kb, at_rows, :] = block
            put_transposed(xt_all, k * (TR // LANE), kb, block)
        if k == 0:
            pl.semaphore_wait(barrier, 3)
        col(k).start()
        img(k).start()
        own(k).start()

    scale2, bias2 = scal[0], scal[1]
    stats[...] = jnp.zeros_like(stats)
    v_all[...] = jnp.zeros_like(v_all)

    def cat(ref, first, count, rows_at):
        return jnp.concatenate([ref[first + q, rows_at, :] for q in range(count)], axis=1)

    def aligned(start, size):
        return pl.ds(start if isinstance(start, int) else pl.multiple_of(start, size), size)

    every = pl.ds(0, dim)

    def sim_pieces(code, slot):
        r, g = code // 8, code % 8

        def piece(k):
            texts = cat(yt_all, g * 2 * cblk + k * cblk, cblk, every)
            images = cat(x_all, 0, kblk, aligned(r * TR, TR))
            sim[slot][:, k * HALF:(k + 1) * HALF] = jnp.dot(images, texts, preferred_element_type=F32)

        return [functools.partial(piece, k) for k in range(2)]

    def grad_pieces(code, slot):
        r, g = code // 8, code % 8

        def img_piece():
            u_all[:, aligned(r * TR, TR)] += lax.dot_general(
                cat(yt_all, g * 2 * cblk, 2 * cblk, every), cat(wgt[slot], 0, 2 * cblk, pl.ds(0, TR)),
                (((1,), (1,)), ((), ())), preferred_element_type=F32)

        def txt_piece(k):
            v_all[:, aligned(g * TC + k * HALF, HALF)] += jnp.dot(
                cat(xt_all, r * (TR // LANE), TR // LANE, every), cat(wgt[slot], k * cblk, cblk, pl.ds(0, TR)),
                preferred_element_type=F32)

        return [img_piece] + [functools.partial(txt_piece, k) for k in range(2)]

    def weight_pieces(code, slot, count, diag):
        blocks = [(r, c) for r in range(0, TR, HR) for c in range(0, TC, HC)]
        per = -(-len(blocks) // count)
        sums = [None] * 4
        if diag:
            tr, tg = code // 8, code % 8
            offset = jnp.where(tr == tg, 0, 4 * TC)
            lag = lax.broadcasted_iota(jnp.int32, (HR, HC), 1) - lax.broadcasted_iota(jnp.int32, (HR, HC), 0)

        def fold(q):
            return jnp.sum(q.reshape(HR // 8, 8, HC), axis=0)

        def piece(k):
            for r, c in blocks[k * per:(k + 1) * per]:
                on_diag = diag and c < HALF and r < c + HC and c < r + HR
                s = sim[slot][r:r + HR, c:c + HC]
                logit2 = s * scale2 + bias2
                if on_diag:
                    same = lag == r - c + offset
                    logit2 = jnp.where(same, -logit2, logit2)
                clamped = jnp.minimum(logit2, CLAMP)
                e = jnp.exp2(clamped)
                v = 1.0 + e
                inv = 1.0 / v
                h = e * inv
                kept = (v - 1.0) * inv
                if on_diag:
                    signed = jnp.where(same, -h, h)
                    kept = kept - h + signed
                    h = signed
                hb = h.astype(BF16)
                for cc in range(0, HC, LANE):
                    wgt[slot][(c + cc) // LANE, r:r + HR, :] = hb[:, cc:cc + LANE]
                for q, part in enumerate((jnp.log2(v) + (logit2 - clamped), kept, h, h * s)):
                    part = fold(part)
                    sums[q] = part if sums[q] is None else sums[q] + part
            if k == count - 1:
                for q in range(4):
                    stats[q] += sums[q]

        return [functools.partial(piece, k) for k in range(count)]

    def step(now, later, slot, diag):
        mxu = sim_pieces(later[slot], slot) + grad_pieces(now[slot], slot)
        vpu = weight_pieces((now[1], later[0])[slot], 1 - slot, len(mxu), diag)
        for a, b in zip(mxu, vpu):
            a()
            b()

    def take_img(k):
        img(k).wait_recv()
        for kb in range(kblk):
            put_transposed(xt_all, nblk + k * (TR // LANE), kb, x_all[kb, rows + k * TR:rows + (k + 1) * TR, :])

    def pass_on(k):
        col(k).wait_recv()
        fwd(k).start()

    def add_part(k):
        q_send(k).wait_recv()
        v_all[:, (SEG + k) * TC:(SEG + k) * TC + HALF] += v_part[k % 2]
        if k + 2 < SEG:
            pl.semaphore_signal(free_sem, inc=1, device_id=(core_nbr,), device_id_type=MESH)

    def send_part(k):
        if k >= 2:
            pl.semaphore_wait(free_sem, 1)
        q_send(k).start()

    events = {}

    def at(trip, fn, k):
        events.setdefault(trip, []).append(functools.partial(fn, k))

    for k in range(SEG):
        if k >= 2:
            at((first_use(lambda r, g: g == k) - 2) // 2, lambda k: own(k).wait_recv(), k)
        at(FORWARD_TRIP[k], pass_on, k)
        use = (first_use(lambda r, g: g == SEG + k) - 2) // 2
        assert use > FORWARD_TRIP[k]
        at(use, lambda k: fwd(k).wait_recv(), k)
        at((first_use(lambda r, g: r == SEG + k) - 2) // 2, take_img, k)
        at(last_use(lambda r, g: g == k) // 2 + 1, lambda k: b_send(k).start(), k)
    for k in range(SEG):
        at(last_use(lambda r, g: r == SEG + k) // 2 + 1, lambda k: u_send(k).start(), k)
        done = last_use(lambda r, g: g == SEG + k) // 2 + 1
        at(done, send_part, k)
        at(done + 1, add_part, k)
    for k in range(SEG):
        at(last_use(lambda r, g: g == SEG + k) // 2 + 2, lambda k: v_send(k).start(), k)
    tail_events = [fn for trip in sorted(events) if trip >= NT // 2 - 1 for fn in events[trip]]

    def trips(first, last, diag):
        def body(p, now):
            for start in range(first, last, 8):
                inside = [trip for trip in range(start, min(start + 8, last)) if trip in events]

                @pl.when((p >= start) & (p < start + 8))
                def _():
                    for trip in inside:
                        @pl.when(p == trip)
                        def _():
                            for fn in events[trip]:
                                fn()
            later = (code_at(p + 1, 0), code_at(p + 1, 1))
            step(now, later, 0, diag)
            step(now, later, 1, diag)
            return later

        lax.fori_loop(first, last, body, (jnp.int32(code_at(first, 0)), jnp.int32(code_at(first, 1))))

    for k in range(2):
        own(k).wait_recv()
        for piece in sim_pieces(code_at(0, k), k):
            piece()
        if k == 0:
            for piece in weight_pieces(code_at(0, 0), 0, 1, True):
                piece()
    last = NT // 2 - 1
    trips(0, DIAG_TRIPS, True)
    trips(DIAG_TRIPS, last, False)
    for piece in (grad_pieces(code_at(last, 0), 0) + weight_pieces(code_at(last, 1), 1, 1, False)
                  + grad_pieces(code_at(last, 1), 1)):
        piece()
    for fn in tail_events:
        fn()

    early = SEG - 1

    def fetch(src, k, slot):
        return pltpu.make_async_copy(src.at[:, pl.ds(k * HALF, HALF)], v_part.at[slot], in_sem.at[slot])

    jobs = []
    for k in range(early):
        jobs += [(u_send, u_in, k), (v_send, v_in, k)]
        if k < SEG - 2:
            jobs.append((b_send, vp_in, k))
    jobs += [(b_send, vp_in, k) for k in range(SEG - 2, SEG)]

    def begin(j):
        make, src, k = jobs[j]
        make(k).wait_recv()
        fetch(src, k, j % 2).start()

    def put(k, is_txt):
        if is_txt:
            return pltpu.make_async_copy(v_all.at[:, pl.ds(k * TC, HALF)], v_out.at[:, pl.ds(k * HALF, HALF)],
                                         out_sem.at[k])
        return pltpu.make_async_copy(u_all.at[:, pl.ds(k * TR, TR)], u_out.at[:, pl.ds(k * TR, TR)],
                                     out_sem.at[SEG + k])

    begin(0)
    for j, (make, src, k) in enumerate(jobs):
        fetch(src, k, j % 2).wait()
        if j + 1 < len(jobs):
            begin(j + 1)
        if make is u_send:
            u_all[:, k * TR:(k + 1) * TR] += v_part[j % 2]
        else:
            v_all[:, k * TC:k * TC + HALF] += v_part[j % 2]
    total = stats[:, :, :LANE]
    for c in range(LANE, HC, LANE):
        total += stats[:, :, c:c + LANE]
    for k in range(3):
        total = swap(k, total)
    for k in range(SEG):
        put(k, False).start()
        put(k, True).start()
    for q in range(4):
        sums_out[q] = jnp.sum(total[q])
    for k in range(SEG):
        put(k, False).wait()
        put(k, True).wait()
    for k in range(SEG):
        img(k).wait_send()
        own(k).wait_send()
        col(k).wait_send()
        fwd(k).wait_send()
        q_send(k).wait_send()
        for copy in (u_send(k), v_send(k), b_send(k)):
            copy.wait_send()
    u_send(early).wait_recv()
    v_send(early).wait_recv()


def finish(first_late, temp, img, txt, u_own, u_in, v_own, v_in, img_out, txt_out):
    def project(emb, total, out):
        emb32 = emb[...].astype(F32)
        inv_norm = lax.rsqrt(jnp.sum(emb32 * emb32, axis=-1, keepdims=True))
        unit_rows = emb32 * inv_norm
        grad_dir = (total * temp[0]).T
        radial = jnp.sum(unit_rows * grad_dir, axis=-1, keepdims=True)
        out[...] = (grad_dir - unit_rows * radial) * inv_norm

    late = pl.program_id(0) >= first_late

    @pl.when(late)
    def _():
        project(img, u_own[...] + u_in[...], img_out)
        project(txt, v_own[...] + v_in[...], txt_out)

    @pl.when(jnp.logical_not(late))
    def _():
        project(img, u_own[...], img_out)
        project(txt, v_own[...], txt_out)


def solution(mesh):
    group_size = mesh.shape['dp']

    def local_fn(img_emb, txt_emb, log_temp, logit_bias):
        rows, dim = img_emb.shape
        total_rows = rows * group_size
        temp_scale = jnp.exp(log_temp)
        scal = jnp.stack([temp_scale * LOG2E, logit_bias * LOG2E])
        nblk, kblk = rows // LANE, dim // LANE
        half_out = jax.ShapeDtypeStruct((dim, rows), F32)
        any_spec = pl.BlockSpec(memory_space=pl.ANY)
        smem_spec = pl.BlockSpec(memory_space=pltpu.SMEM)
        dma = pltpu.SemaphoreType.DMA
        u_own, v_own, u_in, v_in, _, sums = pl.pallas_call(
            kernel,
            out_shape=[half_out] * 5 + [jax.ShapeDtypeStruct((4,), F32)],
            in_specs=[smem_spec] + [any_spec] * 2,
            out_specs=[any_spec] * 5 + [smem_spec],
            scratch_shapes=[
                pltpu.VMEM((4, 8, HC), F32),
                pltpu.VMEM((3, 4, 8, LANE), F32),
                pltpu.VMEM((3, 4, 8, LANE), F32),
                pltpu.VMEM((kblk, 2 * rows, LANE), BF16),
                pltpu.VMEM((2 * nblk, dim, LANE), BF16),
                pltpu.VMEM((4 * nblk, dim, LANE), BF16),
                pltpu.VMEM((dim, 2 * rows), F32),
                pltpu.VMEM((dim, 4 * rows), F32),
                pltpu.VMEM((TR, TC), F32),
                pltpu.VMEM((TR, TC), F32),
                pltpu.VMEM((TC // LANE, TR, LANE), BF16),
                pltpu.VMEM((TC // LANE, TR, LANE), BF16),
                pltpu.VMEM((2, dim, HALF), F32),
                dma((kblk,)),
                dma((SEG * kblk,)),
            ] + [dma((SEG,))] * 16 + [dma((2 * SEG,)), dma((3,)), dma((3,)), dma((2,)), pltpu.SemaphoreType.REGULAR],
            compiler_params=pltpu.CompilerParams(
                collective_id=0, has_side_effects=True, vmem_limit_bytes=67043328),
        )(scal, img_emb, txt_emb)
        sums = sums / total_rows
        loss = LN2 * sums[0] + (sums[2] - sums[1])
        step_rows = 256
        first_late = (SEG - 1) * TR // step_rows
        emb_spec = pl.BlockSpec((step_rows, dim), lambda i: (i, 0))
        col_spec = pl.BlockSpec((dim, step_rows), lambda i: (0, i))
        late_spec = pl.BlockSpec((dim, step_rows), lambda i: (0, jnp.maximum(i, first_late)))
        grad_img, grad_txt = pl.pallas_call(
            functools.partial(finish, first_late),
            grid=(rows // step_rows,),
            out_shape=[jax.ShapeDtypeStruct((rows, dim), F32)] * 2,
            in_specs=[smem_spec] + [emb_spec] * 2 + [col_spec, late_spec] * 2,
            out_specs=[emb_spec] * 2,
        )(temp_scale[None], img_emb, txt_emb, u_own, u_in, v_own, v_in)
        return loss, grad_img, grad_txt, temp_scale * sums[3], sums[2]

    return jax.shard_map(
        local_fn,
        mesh=mesh,
        in_specs=(P('dp', None), P('dp', None), P(), P()),
        out_specs=(P(), P('dp', None), P('dp', None), P(), P()),
        check_vma=False,
    )
```

```python
import functools

import jax
import jax.numpy as jnp
from jax import lax
from jax.experimental import pallas as pl
from jax.experimental.pallas import tpu as pltpu
from jax.sharding import PartitionSpec as P

F32, BF16 = jnp.float32, jnp.bfloat16
MESH = pl.DeviceIdType.MESH
LOG2E = 1.4426950408889634
LN2 = 0.6931471805599453
CLAMP = 64.0
TR, TC, LANE = 512, 1024, 128
HALF = TC // 2
HR, HC = 64, 128
SEG = 4

ORDER = [
    (0, 0), (1, 1), (2, 2), (3, 3), (0, 1), (1, 0), (4, 0), (4, 1),
    (4, 2), (4, 3), (0, 4), (1, 4), (2, 4), (3, 4), (4, 4), (5, 4),
    (4, 5), (6, 4), (4, 6), (5, 0), (5, 1), (5, 5), (7, 4), (5, 6),
    (4, 7), (5, 2), (5, 3), (5, 7), (0, 5), (1, 5), (2, 5), (3, 5),
    (6, 5), (7, 5), (6, 0), (6, 1), (6, 2), (6, 3), (6, 6), (6, 7),
    (0, 6), (1, 6), (2, 6), (3, 6), (7, 6), (7, 7), (7, 0), (7, 1),
    (7, 2), (7, 3), (0, 7), (1, 7), (2, 7), (3, 7), (2, 0), (3, 0),
    (2, 1), (3, 1), (0, 2), (1, 2), (3, 2), (0, 3), (1, 3), (2, 3),
]
assert len(set(ORDER)) == 64
NT = len(ORDER)
DIAG_TRIPS = 2
FORWARD_TRIP = (2, 6, 7, 10)


def code_at(trip, parity):
    codes = [8 * r + g for r, g in ORDER[parity::2]]
    if isinstance(trip, int):
        return codes[trip]
    code = jnp.int32(codes[0])
    for k, value in enumerate(codes[1:], 1):
        code = jnp.where(trip == k, value, code)
    return code


def last_use(match):
    return max(t for t, rg in enumerate(ORDER) if match(*rg))


def first_use(match):
    return min(t for t, rg in enumerate(ORDER) if match(*rg))


def kernel(total_rows, scal, img_hbm, txt_hbm, u_out, v_out, u_in, v_in, vp_in, loss_out, temp_out, bias_out, stats, st_buf, st_in, x_all, xt_all, yt_all, u_all, v_all,
           s0, s1, h0, h1, v_part, x_sem, y_sem, img_s, img_r, own_s, own_r, col_s, col_r, fwd_s, fwd_r, u_s, u_r,
           q_s, q_r, v_s, v_r, b_s, b_r, out_sem, st_s, st_r, in_sem, free_sem):
    me = lax.axis_index('dp')
    core_nbr, row_nbr, col_nbr = me ^ 1, me ^ 2, me ^ 4
    dim = u_all.shape[0]
    rows = img_hbm.shape[0]
    nblk = rows // LANE
    cblk = HALF // LANE
    kblk = dim // LANE

    barrier = pltpu.get_barrier_semaphore()
    for nbr in (core_nbr, row_nbr, col_nbr):
        pl.semaphore_signal(barrier, inc=1, device_id=(nbr,), device_id_type=MESH)

    def remote(src, dst, s, r, k, dev):
        return pltpu.make_async_remote_copy(src_ref=src, dst_ref=dst, send_sem=s.at[k], recv_sem=r.at[k],
                                            device_id=(dev,), device_id_type=MESH)

    def img(k):
        return remote(x_all.at[:, pl.ds(k * TR, TR)], x_all.at[:, pl.ds(rows + k * TR, TR)], img_s, img_r, k, row_nbr)

    def own(k):
        return remote(yt_all.at[pl.ds(k * 2 * cblk, cblk)], yt_all.at[pl.ds(k * 2 * cblk + cblk, cblk)], own_s, own_r, k,
                      core_nbr)

    def col(k):
        return remote(yt_all.at[pl.ds(k * 2 * cblk, cblk)], yt_all.at[pl.ds((SEG + k) * 2 * cblk, cblk)], col_s, col_r, k,
                      col_nbr)

    def fwd(k):
        return remote(yt_all.at[pl.ds((SEG + k) * 2 * cblk, cblk)], yt_all.at[pl.ds((SEG + k) * 2 * cblk + cblk, cblk)],
                      fwd_s, fwd_r, k, core_nbr)

    def u_send(k):
        return remote(u_all.at[:, pl.ds(rows + k * TR, TR)], u_in.at[:, pl.ds(k * TR, TR)], u_s, u_r, k, row_nbr)

    def q_send(k):
        return remote(v_all.at[:, pl.ds((SEG + k) * TC + HALF, HALF)], v_part.at[k % 2], q_s, q_r, k, core_nbr)

    def v_send(k):
        return remote(v_all.at[:, pl.ds((SEG + k) * TC, HALF)], v_in.at[:, pl.ds(k * HALF, HALF)], v_s, v_r, k, col_nbr)

    def b_send(k):
        return remote(v_all.at[:, pl.ds(k * TC + HALF, HALF)], vp_in.at[:, pl.ds(k * HALF, HALF)], b_s, b_r, k, core_nbr)

    def load_img(kb):
        return pltpu.make_async_copy(img_hbm.at[:, pl.ds(kb * LANE, LANE)], x_all.at[kb, pl.ds(0, rows)], x_sem.at[kb])

    def load_txt(k, kb):
        return pltpu.make_async_copy(txt_hbm.at[pl.ds(k * TR, TR), pl.ds(kb * LANE, LANE)],
                                     wgt[k % 2].at[kb], y_sem.at[k * kblk + kb])

    def swap(k, value):
        nbr = (core_nbr, row_nbr, col_nbr)[k]
        st_buf[k] = value
        copy = remote(st_buf.at[k], st_in.at[k], st_s, st_r, k, nbr)
        copy.start()
        copy.wait()
        return st_buf[k] + st_in[k]

    def load_img(kb):
        return pltpu.make_async_copy(img_hbm.at[:, pl.ds(kb * LANE, LANE)], x_all.at[kb, pl.ds(0, rows)], x_sem.at[kb])

    def load_txt(k, kb):
        return pltpu.make_async_copy(txt_hbm.at[pl.ds(k * TR, TR), pl.ds(kb * LANE, LANE)],
                                     wgt[k % 2].at[kb], y_sem.at[k * kblk + kb])

    def swap(k, value):
        nbr = (core_nbr, row_nbr, col_nbr)[k]
        st_buf[k] = value
        copy = remote(st_buf.at[k], st_in.at[k], st_s, st_r, k, nbr)
        copy.start()
        copy.wait()
        return st_buf[k] + st_in[k]

    def store(k):
        if k < SEG:
            return pltpu.make_async_copy(v_all.at[:, pl.ds(k * TC, HALF)], v_out.at[:, pl.ds(k * HALF, HALF)],
                                         out_sem.at[k])
        return pltpu.make_async_copy(u_all.at[:, pl.ds(0, rows)], u_out, out_sem.at[k])

    sim, wgt = (s0, s1), (h0, h1)
    for kb in range(kblk):
        load_txt(0, kb).start()
    for kb in range(kblk):
        load_img(kb).start()
    for kb in range(kblk):
        load_txt(1, kb).start()

    u_all[...] = jnp.zeros_like(u_all)

    def unit(blocks):
        wide = [block.astype(F32) for block in blocks]
        norm2 = jnp.sum(functools.reduce(jnp.add, [w * w for w in wide]), axis=-1, keepdims=True)
        inv_norm = lax.rsqrt(norm2)
        return [(w * inv_norm).astype(BF16) for w in wide]

    def put_transposed(ref, first, kb, block):
        flipped = block.T
        for q in range(TR // LANE):
            ref[first + q, kb * LANE:(kb + 1) * LANE, :] = flipped[:, q * LANE:(q + 1) * LANE]

    for k in range(SEG):
        for kb in range(kblk):
            load_txt(k, kb).wait()
        for kb, block in enumerate(unit([wgt[k % 2][kb] for kb in range(kblk)])):
            put_transposed(yt_all, k * 2 * cblk, kb, block)
        if k == 0:
            for kb in range(kblk):
                load_img(kb).wait()
        if k + 2 < SEG:
            for kb in range(kblk):
                load_txt(k + 2, kb).start()
        at_rows = slice(k * TR, (k + 1) * TR)
        for kb, block in enumerate(unit([x_all[kb, at_rows, :] for kb in range(kblk)])):
            x_all[kb, at_rows, :] = block
            put_transposed(xt_all, k * (TR // LANE), kb, block)
        if k == 0:
            pl.semaphore_wait(barrier, 3)
        col(k).start()
        img(k).start()
        own(k).start()

    scale2, bias2 = scal[0] * LOG2E, scal[1] * LOG2E
    stats[...] = jnp.zeros_like(stats)
    v_all[...] = jnp.zeros_like(v_all)

    def cat(ref, first, count, rows_at):
        return jnp.concatenate([ref[first + q, rows_at, :] for q in range(count)], axis=1)

    def aligned(start, size):
        return pl.ds(start if isinstance(start, int) else pl.multiple_of(start, size), size)

    every = pl.ds(0, dim)

    def sim_pieces(code, slot):
        r, g = code // 8, code % 8

        def piece(k):
            texts = cat(yt_all, g * 2 * cblk + k * cblk, cblk, every)
            images = cat(x_all, 0, kblk, aligned(r * TR, TR))
            sim[slot][:, k * HALF:(k + 1) * HALF] = jnp.dot(images, texts, preferred_element_type=F32)

        return [functools.partial(piece, k) for k in range(2)]

    def grad_pieces(code, slot):
        r, g = code // 8, code % 8

        def img_piece():
            u_all[:, aligned(r * TR, TR)] += lax.dot_general(
                cat(yt_all, g * 2 * cblk, 2 * cblk, every), cat(wgt[slot], 0, 2 * cblk, pl.ds(0, TR)),
                (((1,), (1,)), ((), ())), preferred_element_type=F32)

        def txt_piece(k):
            v_all[:, aligned(g * TC + k * HALF, HALF)] += jnp.dot(
                cat(xt_all, r * (TR // LANE), TR // LANE, every), cat(wgt[slot], k * cblk, cblk, pl.ds(0, TR)),
                preferred_element_type=F32)

        return [img_piece] + [functools.partial(txt_piece, k) for k in range(2)]

    def weight_pieces(code, slot, count, diag):
        blocks = [(r, c) for r in range(0, TR, HR) for c in range(0, TC, HC)]
        per = -(-len(blocks) // count)
        sums = [None] * 4
        if diag:
            tr, tg = code // 8, code % 8
            offset = jnp.where(tr == tg, 0, 4 * TC)
            lag = lax.broadcasted_iota(jnp.int32, (HR, HC), 1) - lax.broadcasted_iota(jnp.int32, (HR, HC), 0)

        def fold(q):
            return jnp.sum(q.reshape(HR // 8, 8, HC), axis=0)

        def piece(k):
            for r, c in blocks[k * per:(k + 1) * per]:
                on_diag = diag and c < HALF and r < c + HC and c < r + HR
                s = sim[slot][r:r + HR, c:c + HC]
                logit2 = s * scale2 + bias2
                if on_diag:
                    same = lag == r - c + offset
                    logit2 = jnp.where(same, -logit2, logit2)
                clamped = jnp.minimum(logit2, CLAMP)
                e = jnp.exp2(clamped)
                v = 1.0 + e
                inv = 1.0 / v
                h = e * inv
                kept = (v - 1.0) * inv
                if on_diag:
                    signed = jnp.where(same, -h, h)
                    kept = kept - h + signed
                    h = signed
                hb = h.astype(BF16)
                for cc in range(0, HC, LANE):
                    wgt[slot][(c + cc) // LANE, r:r + HR, :] = hb[:, cc:cc + LANE]
                for q, part in enumerate((jnp.log2(v) + (logit2 - clamped), kept, h, h * s)):
                    part = fold(part)
                    sums[q] = part if sums[q] is None else sums[q] + part
            if k == count - 1:
                for q in range(4):
                    stats[q] += sums[q]

        return [functools.partial(piece, k) for k in range(count)]

    def step(now, later, slot, diag):
        mxu = sim_pieces(later[slot], slot) + grad_pieces(now[slot], slot)
        vpu = weight_pieces((now[1], later[0])[slot], 1 - slot, len(mxu), diag)
        for a, b in zip(mxu, vpu):
            a()
            b()

    def take_img(k):
        img(k).wait_recv()
        for kb in range(kblk):
            put_transposed(xt_all, nblk + k * (TR // LANE), kb, x_all[kb, rows + k * TR:rows + (k + 1) * TR, :])

    def pass_on(k):
        col(k).wait_recv()
        fwd(k).start()

    def add_part(k):
        q_send(k).wait_recv()
        v_all[:, (SEG + k) * TC:(SEG + k) * TC + HALF] += v_part[k % 2]
        if k + 2 < SEG:
            pl.semaphore_signal(free_sem, inc=1, device_id=(core_nbr,), device_id_type=MESH)

    def send_part(k):
        if k >= 2:
            pl.semaphore_wait(free_sem, 1)
        q_send(k).start()

    events = {}

    def at(trip, fn, k):
        events.setdefault(trip, []).append(functools.partial(fn, k))

    for k in range(SEG):
        if k >= 2:
            at((first_use(lambda r, g: g == k) - 2) // 2, lambda k: own(k).wait_recv(), k)
        at(FORWARD_TRIP[k], pass_on, k)
        use = (first_use(lambda r, g: g == SEG + k) - 2) // 2
        assert use > FORWARD_TRIP[k]
        at(use, lambda k: fwd(k).wait_recv(), k)
        at((first_use(lambda r, g: r == SEG + k) - 2) // 2, take_img, k)
        at(last_use(lambda r, g: g == k) // 2 + 1, lambda k: b_send(k).start(), k)
    for k in range(SEG):
        at(last_use(lambda r, g: r == SEG + k) // 2 + 1, lambda k: u_send(k).start(), k)
        done = last_use(lambda r, g: g == SEG + k) // 2 + 1
        at(done, send_part, k)
        at(done + 1, add_part, k)
    for k in range(SEG):
        at(last_use(lambda r, g: g == SEG + k) // 2 + 2, lambda k: v_send(k).start(), k)
    tail_events = [fn for trip in sorted(events) if trip >= NT // 2 - 1 for fn in events[trip]]

    def trips(first, last, diag):
        def body(p, now):
            for start in range(first, last, 8):
                inside = [trip for trip in range(start, min(start + 8, last)) if trip in events]

                @pl.when((p >= start) & (p < start + 8))
                def _():
                    for trip in inside:
                        @pl.when(p == trip)
                        def _():
                            for fn in events[trip]:
                                fn()
            later = (code_at(p + 1, 0), code_at(p + 1, 1))
            step(now, later, 0, diag)
            step(now, later, 1, diag)
            return later

        lax.fori_loop(first, last, body, (jnp.int32(code_at(first, 0)), jnp.int32(code_at(first, 1))))

    for k in range(2):
        own(k).wait_recv()
        for piece in sim_pieces(code_at(0, k), k):
            piece()
        if k == 0:
            for piece in weight_pieces(code_at(0, 0), 0, 1, True):
                piece()
    last = NT // 2 - 1
    trips(0, DIAG_TRIPS, True)
    trips(DIAG_TRIPS, last, False)
    for piece in (grad_pieces(code_at(last, 0), 0) + weight_pieces(code_at(last, 1), 1, 1, False)
                  + grad_pieces(code_at(last, 1), 1)):
        piece()
    for fn in tail_events:
        fn()

    early = SEG - 1

    def fetch(src, k, slot):
        return pltpu.make_async_copy(src.at[:, pl.ds(k * HALF, HALF)], v_part.at[slot], in_sem.at[slot])

    jobs = []
    for k in range(early):
        jobs += [(u_send, u_in, k), (v_send, v_in, k)]
        if k < SEG - 2:
            jobs.append((b_send, vp_in, k))
    jobs += [(b_send, vp_in, k) for k in range(SEG - 2, SEG)]

    def begin(j):
        make, src, k = jobs[j]
        make(k).wait_recv()
        fetch(src, k, j % 2).start()

    def put(k, is_txt):
        if is_txt:
            return pltpu.make_async_copy(v_all.at[:, pl.ds(k * TC, HALF)], v_out.at[:, pl.ds(k * HALF, HALF)],
                                         out_sem.at[k])
        return pltpu.make_async_copy(u_all.at[:, pl.ds(k * TR, TR)], u_out.at[:, pl.ds(k * TR, TR)],
                                     out_sem.at[SEG + k])

    begin(0)
    total = stats[:, :, :LANE]
    for c in range(LANE, HC, LANE):
        total += stats[:, :, c:c + LANE]
    for k in range(3):
        total = swap(k, total)
    sums = [jnp.sum(total[q]) / total_rows for q in range(4)]
    loss_out[0] = LN2 * sums[0] + (sums[2] - sums[1])
    temp_out[0] = scal[0] * sums[3]
    bias_out[0] = sums[2]
    for j, (make, src, k) in enumerate(jobs):
        fetch(src, k, j % 2).wait()
        if j + 1 < len(jobs):
            begin(j + 1)
        if make is u_send:
            u_all[:, k * TR:(k + 1) * TR] += v_part[j % 2]
        else:
            v_all[:, k * TC:k * TC + HALF] += v_part[j % 2]
        rest = [job[2] for job in jobs[j + 1:] if (job[0] is u_send) == (make is u_send)]
        if k not in rest:
            put(k, make is not u_send).start()
    put(early, False).start()
    for k in range(SEG):
        put(k, False).wait()
        put(k, True).wait()
    for k in range(SEG):
        img(k).wait_send()
        own(k).wait_send()
        col(k).wait_send()
        fwd(k).wait_send()
        q_send(k).wait_send()
        for copy in (u_send(k), v_send(k), b_send(k)):
            copy.wait_send()
    u_send(early).wait_recv()
    v_send(early).wait_recv()


def finish(first_late, scal, img, txt, u_own, u_in, v_own, v_in, img_out, txt_out):
    def project(emb, total, out):
        emb32 = emb[...].astype(F32)
        inv_norm = lax.rsqrt(jnp.sum(emb32 * emb32, axis=-1, keepdims=True))
        unit_rows = emb32 * inv_norm
        grad_dir = (total * scal[0]).T
        radial = jnp.sum(unit_rows * grad_dir, axis=-1, keepdims=True)
        out[...] = (grad_dir - unit_rows * radial) * inv_norm

    late = pl.program_id(0) >= first_late

    @pl.when(late)
    def _():
        project(img, u_own[...] + u_in[...], img_out)
        project(txt, v_own[...] + v_in[...], txt_out)

    @pl.when(jnp.logical_not(late))
    def _():
        project(img, u_own[...], img_out)
        project(txt, v_own[...], txt_out)


def solution(mesh):
    group_size = mesh.shape['dp']

    def local_fn(img_emb, txt_emb, log_temp, logit_bias):
        rows, dim = img_emb.shape
        total_rows = rows * group_size
        scal = jnp.stack([jnp.exp(log_temp), logit_bias])
        nblk, kblk = rows // LANE, dim // LANE
        half_out = jax.ShapeDtypeStruct((dim, rows), F32)
        any_spec = pl.BlockSpec(memory_space=pl.ANY)
        smem_spec = pl.BlockSpec(memory_space=pltpu.SMEM)
        dma = pltpu.SemaphoreType.DMA
        u_own, v_own, u_in, v_in, _, loss, grad_temp, grad_bias = pl.pallas_call(
            functools.partial(kernel, float(total_rows)),
            out_shape=[half_out] * 5 + [jax.ShapeDtypeStruct((1,), F32)] * 3,
            in_specs=[smem_spec] + [any_spec] * 2,
            out_specs=[any_spec] * 5 + [smem_spec] * 3,
            scratch_shapes=[
                pltpu.VMEM((4, 8, HC), F32),
                pltpu.VMEM((3, 4, 8, LANE), F32),
                pltpu.VMEM((3, 4, 8, LANE), F32),
                pltpu.VMEM((kblk, 2 * rows, LANE), BF16),
                pltpu.VMEM((2 * nblk, dim, LANE), BF16),
                pltpu.VMEM((4 * nblk, dim, LANE), BF16),
                pltpu.VMEM((dim, 2 * rows), F32),
                pltpu.VMEM((dim, 4 * rows), F32),
                pltpu.VMEM((TR, TC), F32),
                pltpu.VMEM((TR, TC), F32),
                pltpu.VMEM((TC // LANE, TR, LANE), BF16),
                pltpu.VMEM((TC // LANE, TR, LANE), BF16),
                pltpu.VMEM((2, dim, HALF), F32),
                dma((kblk,)),
                dma((SEG * kblk,)),
            ] + [dma((SEG,))] * 16 + [dma((2 * SEG,)), dma((3,)), dma((3,)), dma((2,)), pltpu.SemaphoreType.REGULAR],
            compiler_params=pltpu.CompilerParams(
                collective_id=0, has_side_effects=True, vmem_limit_bytes=67043328),
        )(scal, img_emb, txt_emb)
        step_rows = 256
        first_late = (SEG - 1) * TR // step_rows
        emb_spec = pl.BlockSpec((step_rows, dim), lambda i: (i, 0))
        col_spec = pl.BlockSpec((dim, step_rows), lambda i: (0, i))
        late_spec = pl.BlockSpec((dim, step_rows), lambda i: (0, jnp.maximum(i, first_late)))
        grad_img, grad_txt = pl.pallas_call(
            functools.partial(finish, first_late),
            grid=(rows // step_rows,),
            out_shape=[jax.ShapeDtypeStruct((rows, dim), F32)] * 2,
            in_specs=[smem_spec] + [emb_spec] * 2 + [col_spec, late_spec] * 2,
            out_specs=[emb_spec] * 2,
        )(scal, img_emb, txt_emb, u_own, u_in, v_own, v_in)
        return loss[0], grad_img, grad_txt, grad_temp[0], grad_bias[0]

    return jax.shard_map(
        local_fn,
        mesh=mesh,
        in_specs=(P('dp', None), P('dp', None), P(), P()),
        out_specs=(P(), P('dp', None), P('dp', None), P(), P()),
        check_vma=False,
    )
```

```python
import functools

import jax
import jax.numpy as jnp
from jax import lax
from jax.experimental import pallas as pl
from jax.experimental.pallas import tpu as pltpu
from jax.sharding import PartitionSpec as P

F32, BF16 = jnp.float32, jnp.bfloat16
MESH = pl.DeviceIdType.MESH
LOG2E = 1.4426950408889634
LN2 = 0.6931471805599453
CLAMP = 64.0
TR, TC, LANE = 512, 1024, 128
HALF = TC // 2
HR, HC = 64, 128
SEG = 4

ORDER = [
    (0, 0), (1, 1), (2, 2), (3, 3), (0, 1), (1, 0), (4, 0), (4, 1),
    (4, 2), (4, 3), (0, 4), (1, 4), (2, 4), (3, 4), (4, 4), (5, 4),
    (4, 5), (6, 4), (4, 6), (5, 0), (5, 1), (5, 5), (7, 4), (5, 6),
    (4, 7), (5, 2), (5, 3), (5, 7), (0, 5), (1, 5), (2, 5), (3, 5),
    (6, 5), (7, 5), (6, 0), (6, 1), (6, 2), (6, 3), (6, 6), (6, 7),
    (0, 6), (1, 6), (2, 6), (3, 6), (7, 6), (7, 7), (7, 0), (7, 1),
    (7, 2), (7, 3), (0, 7), (1, 7), (2, 7), (3, 7), (2, 0), (3, 0),
    (2, 1), (3, 1), (0, 2), (1, 2), (3, 2), (0, 3), (1, 3), (2, 3),
]
assert len(set(ORDER)) == 64
NT = len(ORDER)
DIAG_TRIPS = 2
FORWARD_TRIP = (2, 6, 7, 10)


def code_at(trip, parity):
    codes = [8 * r + g for r, g in ORDER[parity::2]]
    if isinstance(trip, int):
        return codes[trip]
    code = jnp.int32(codes[0])
    for k, value in enumerate(codes[1:], 1):
        code = jnp.where(trip == k, value, code)
    return code


def last_use(match):
    return max(t for t, rg in enumerate(ORDER) if match(*rg))


def first_use(match):
    return min(t for t, rg in enumerate(ORDER) if match(*rg))


def kernel(total_rows, scal, img_hbm, txt_hbm, u_out, v_out, u_in, v_in, vp_in, loss_out, temp_out, bias_out, stats, st_buf, st_in, x_all, xt_all, yt_all, u_all, v_all,
           s0, s1, h0, h1, v_part, x_sem, y_sem, img_s, img_r, own_s, own_r, col_s, col_r, fwd_s, fwd_r, u_s, u_r,
           q_s, q_r, v_s, v_r, b_s, b_r, out_sem, st_s, st_r, in_sem, free_sem):
    me = lax.axis_index('dp')
    core_nbr, row_nbr, col_nbr, far_nbr = me ^ 1, me ^ 2, me ^ 4, me ^ 6
    dim = u_all.shape[0]
    rows = img_hbm.shape[0]
    nblk = rows // LANE
    cblk = HALF // LANE
    kblk = dim // LANE

    barrier = pltpu.get_barrier_semaphore()
    for nbr in (core_nbr, row_nbr, col_nbr, far_nbr):
        pl.semaphore_signal(barrier, inc=1, device_id=(nbr,), device_id_type=MESH)

    def remote(src, dst, s, r, k, dev):
        return pltpu.make_async_remote_copy(src_ref=src, dst_ref=dst, send_sem=s.at[k], recv_sem=r.at[k],
                                            device_id=(dev,), device_id_type=MESH)

    def img(k):
        return remote(x_all.at[:, pl.ds(k * TR, TR)], x_all.at[:, pl.ds(rows + k * TR, TR)], img_s, img_r, k, row_nbr)

    def own(k):
        return remote(yt_all.at[pl.ds(k * 2 * cblk, cblk)], yt_all.at[pl.ds(k * 2 * cblk + cblk, cblk)], own_s, own_r, k,
                      core_nbr)

    def col(k):
        return remote(yt_all.at[pl.ds(k * 2 * cblk, cblk)], yt_all.at[pl.ds((SEG + k) * 2 * cblk, cblk)], col_s, col_r, k,
                      col_nbr)

    def fwd(k):
        return remote(yt_all.at[pl.ds((SEG + k) * 2 * cblk, cblk)], yt_all.at[pl.ds((SEG + k) * 2 * cblk + cblk, cblk)],
                      fwd_s, fwd_r, k, core_nbr)

    def u_send(k):
        return remote(u_all.at[:, pl.ds(rows + k * TR, TR)], u_in.at[:, pl.ds(k * TR, TR)], u_s, u_r, k, row_nbr)

    def q_send(k):
        return remote(v_all.at[:, pl.ds((SEG + k) * TC + HALF, HALF)], v_part.at[k % 2], q_s, q_r, k, core_nbr)

    def v_send(k):
        return remote(v_all.at[:, pl.ds((SEG + k) * TC, HALF)], v_in.at[:, pl.ds(k * HALF, HALF)], v_s, v_r, k, col_nbr)

    def b_send(k):
        return remote(v_all.at[:, pl.ds(k * TC + HALF, HALF)], vp_in.at[:, pl.ds(k * HALF, HALF)], b_s, b_r, k, core_nbr)

    def load_img(kb):
        return pltpu.make_async_copy(img_hbm.at[:, pl.ds(kb * LANE, LANE)], x_all.at[kb, pl.ds(0, rows)], x_sem.at[kb])

    def load_txt(k, kb):
        return pltpu.make_async_copy(txt_hbm.at[pl.ds(k * TR, TR), pl.ds(kb * LANE, LANE)],
                                     wgt[k % 2].at[kb], y_sem.at[k * kblk + kb])

    def stat_copy(k):
        return remote(st_buf.at[min(k, 1)], st_in.at[k], st_s, st_r, k, (core_nbr, row_nbr, col_nbr, far_nbr)[k])

    sim, wgt = (s0, s1), (h0, h1)
    for kb in range(kblk):
        load_txt(0, kb).start()
    for kb in range(kblk):
        load_img(kb).start()
    for kb in range(kblk):
        load_txt(1, kb).start()

    u_all[...] = jnp.zeros_like(u_all)

    def unit(blocks):
        wide = [block.astype(F32) for block in blocks]
        norm2 = jnp.sum(functools.reduce(jnp.add, [w * w for w in wide]), axis=-1, keepdims=True)
        inv_norm = lax.rsqrt(norm2)
        return [(w * inv_norm).astype(BF16) for w in wide]

    def put_transposed(ref, first, kb, block):
        flipped = block.T
        for q in range(TR // LANE):
            ref[first + q, kb * LANE:(kb + 1) * LANE, :] = flipped[:, q * LANE:(q + 1) * LANE]

    for k in range(SEG):
        for kb in range(kblk):
            load_txt(k, kb).wait()
        for kb, block in enumerate(unit([wgt[k % 2][kb] for kb in range(kblk)])):
            put_transposed(yt_all, k * 2 * cblk, kb, block)
        if k == 0:
            for kb in range(kblk):
                load_img(kb).wait()
        if k + 2 < SEG:
            for kb in range(kblk):
                load_txt(k + 2, kb).start()
        at_rows = slice(k * TR, (k + 1) * TR)
        for kb, block in enumerate(unit([x_all[kb, at_rows, :] for kb in range(kblk)])):
            x_all[kb, at_rows, :] = block
            put_transposed(xt_all, k * (TR // LANE), kb, block)
        if k == 0:
            pl.semaphore_wait(barrier, 4)
        col(k).start()
        img(k).start()
        own(k).start()

    scale2, bias2 = scal[0] * LOG2E, scal[1] * LOG2E
    stats[...] = jnp.zeros_like(stats)
    v_all[...] = jnp.zeros_like(v_all)

    def cat(ref, first, count, rows_at):
        return jnp.concatenate([ref[first + q, rows_at, :] for q in range(count)], axis=1)

    def aligned(start, size):
        return pl.ds(start if isinstance(start, int) else pl.multiple_of(start, size), size)

    every = pl.ds(0, dim)

    def sim_pieces(code, slot):
        r, g = code // 8, code % 8

        def piece(k):
            texts = cat(yt_all, g * 2 * cblk + k * cblk, cblk, every)
            images = cat(x_all, 0, kblk, aligned(r * TR, TR))
            sim[slot][:, k * HALF:(k + 1) * HALF] = jnp.dot(images, texts, preferred_element_type=F32)

        return [functools.partial(piece, k) for k in range(2)]

    def grad_pieces(code, slot):
        r, g = code // 8, code % 8

        def img_piece():
            u_all[:, aligned(r * TR, TR)] += lax.dot_general(
                cat(yt_all, g * 2 * cblk, 2 * cblk, every), cat(wgt[slot], 0, 2 * cblk, pl.ds(0, TR)),
                (((1,), (1,)), ((), ())), preferred_element_type=F32)

        def txt_piece(k):
            v_all[:, aligned(g * TC + k * HALF, HALF)] += jnp.dot(
                cat(xt_all, r * (TR // LANE), TR // LANE, every), cat(wgt[slot], k * cblk, cblk, pl.ds(0, TR)),
                preferred_element_type=F32)

        return [img_piece] + [functools.partial(txt_piece, k) for k in range(2)]

    def weight_pieces(code, slot, count, diag):
        blocks = [(r, c) for r in range(0, TR, HR) for c in range(0, TC, HC)]
        per = -(-len(blocks) // count)
        sums = [None] * 4
        if diag:
            tr, tg = code // 8, code % 8
            offset = jnp.where(tr == tg, 0, 4 * TC)
            lag = lax.broadcasted_iota(jnp.int32, (HR, HC), 1) - lax.broadcasted_iota(jnp.int32, (HR, HC), 0)

        def fold(q):
            return jnp.sum(q.reshape(HR // 8, 8, HC), axis=0)

        def piece(k):
            for r, c in blocks[k * per:(k + 1) * per]:
                on_diag = diag and c < HALF and r < c + HC and c < r + HR
                s = sim[slot][r:r + HR, c:c + HC]
                logit2 = s * scale2 + bias2
                if on_diag:
                    same = lag == r - c + offset
                    logit2 = jnp.where(same, -logit2, logit2)
                clamped = jnp.minimum(logit2, CLAMP)
                e = jnp.exp2(clamped)
                v = 1.0 + e
                inv = 1.0 / v
                h = e * inv
                kept = (v - 1.0) * inv
                if on_diag:
                    signed = jnp.where(same, -h, h)
                    kept = kept - h + signed
                    h = signed
                hb = h.astype(BF16)
                for cc in range(0, HC, LANE):
                    wgt[slot][(c + cc) // LANE, r:r + HR, :] = hb[:, cc:cc + LANE]
                for q, part in enumerate((jnp.log2(v) + (logit2 - clamped), kept, h, h * s)):
                    part = fold(part)
                    sums[q] = part if sums[q] is None else sums[q] + part
            if k == count - 1:
                for q in range(4):
                    stats[q] += sums[q]

        return [functools.partial(piece, k) for k in range(count)]

    def step(now, later, slot, diag):
        mxu = sim_pieces(later[slot], slot) + grad_pieces(now[slot], slot)
        vpu = weight_pieces((now[1], later[0])[slot], 1 - slot, len(mxu), diag)
        for a, b in zip(mxu, vpu):
            a()
            b()

    def take_img(k):
        img(k).wait_recv()
        for kb in range(kblk):
            put_transposed(xt_all, nblk + k * (TR // LANE), kb, x_all[kb, rows + k * TR:rows + (k + 1) * TR, :])

    def pass_on(k):
        col(k).wait_recv()
        fwd(k).start()

    def add_part(k):
        q_send(k).wait_recv()
        v_all[:, (SEG + k) * TC:(SEG + k) * TC + HALF] += v_part[k % 2]
        if k + 2 < SEG:
            pl.semaphore_signal(free_sem, inc=1, device_id=(core_nbr,), device_id_type=MESH)

    def send_part(k):
        if k >= 2:
            pl.semaphore_wait(free_sem, 1)
        q_send(k).start()

    events = {}

    def at(trip, fn, k):
        events.setdefault(trip, []).append(functools.partial(fn, k))

    for k in range(SEG):
        if k >= 2:
            at((first_use(lambda r, g: g == k) - 2) // 2, lambda k: own(k).wait_recv(), k)
        at(FORWARD_TRIP[k], pass_on, k)
        use = (first_use(lambda r, g: g == SEG + k) - 2) // 2
        assert use > FORWARD_TRIP[k]
        at(use, lambda k: fwd(k).wait_recv(), k)
        at((first_use(lambda r, g: r == SEG + k) - 2) // 2, take_img, k)
        at(last_use(lambda r, g: g == k) // 2 + 1, lambda k: b_send(k).start(), k)
    for k in range(SEG):
        at(last_use(lambda r, g: r == SEG + k) // 2 + 1, lambda k: u_send(k).start(), k)
        done = last_use(lambda r, g: g == SEG + k) // 2 + 1
        at(done, send_part, k)
        at(done + 1, add_part, k)
    for k in range(SEG):
        at(last_use(lambda r, g: g == SEG + k) // 2 + 2, lambda k: v_send(k).start(), k)
    tail_events = [fn for trip in sorted(events) if trip >= NT // 2 - 1 for fn in events[trip]]

    def trips(first, last, diag):
        def body(p, now):
            for start in range(first, last, 8):
                inside = [trip for trip in range(start, min(start + 8, last)) if trip in events]

                @pl.when((p >= start) & (p < start + 8))
                def _():
                    for trip in inside:
                        @pl.when(p == trip)
                        def _():
                            for fn in events[trip]:
                                fn()
            later = (code_at(p + 1, 0), code_at(p + 1, 1))
            step(now, later, 0, diag)
            step(now, later, 1, diag)
            return later

        lax.fori_loop(first, last, body, (jnp.int32(code_at(first, 0)), jnp.int32(code_at(first, 1))))

    for k in range(2):
        own(k).wait_recv()
        for piece in sim_pieces(code_at(0, k), k):
            piece()
        if k == 0:
            for piece in weight_pieces(code_at(0, 0), 0, 1, True):
                piece()
    last = NT // 2 - 1
    trips(0, DIAG_TRIPS, True)
    trips(DIAG_TRIPS, last, False)
    for piece in (grad_pieces(code_at(last, 0), 0) + weight_pieces(code_at(last, 1), 1, 1, False)
                  + grad_pieces(code_at(last, 1), 1)):
        piece()
    for fn in tail_events:
        fn()

    early = SEG - 1

    def fetch(src, k, slot):
        return pltpu.make_async_copy(src.at[:, pl.ds(k * HALF, HALF)], v_part.at[slot], in_sem.at[slot])

    jobs = []
    for k in range(early):
        jobs += [(u_send, u_in, k), (v_send, v_in, k)]
        if k < SEG - 2:
            jobs.append((b_send, vp_in, k))
    jobs += [(b_send, vp_in, k) for k in range(SEG - 2, SEG)]

    def begin(j):
        make, src, k = jobs[j]
        make(k).wait_recv()
        fetch(src, k, j % 2).start()

    def put(k, is_txt):
        if is_txt:
            return pltpu.make_async_copy(v_all.at[:, pl.ds(k * TC, HALF)], v_out.at[:, pl.ds(k * HALF, HALF)],
                                         out_sem.at[k])
        return pltpu.make_async_copy(u_all.at[:, pl.ds(k * TR, TR)], u_out.at[:, pl.ds(k * TR, TR)],
                                     out_sem.at[SEG + k])

    begin(0)
    total = stats[:, :, :LANE]
    for c in range(LANE, HC, LANE):
        total += stats[:, :, c:c + LANE]
    st_buf[0] = total
    stat_copy(0).start()
    for j, (make, src, k) in enumerate(jobs):
        fetch(src, k, j % 2).wait()
        if j + 1 < len(jobs):
            begin(j + 1)
        if make is u_send:
            u_all[:, k * TR:(k + 1) * TR] += v_part[j % 2]
        else:
            v_all[:, k * TC:k * TC + HALF] += v_part[j % 2]
        rest = [job[2] for job in jobs[j + 1:] if (job[0] is u_send) == (make is u_send)]
        if k not in rest:
            put(k, make is not u_send).start()
        if j == 5:
            stat_copy(0).wait()
            st_buf[1] = st_buf[0] + st_in[0]
            for q in range(1, 4):
                stat_copy(q).start()
    put(early, False).start()
    for q in range(1, 4):
        stat_copy(q).wait()
    total = (st_buf[1] + st_in[1]) + (st_in[2] + st_in[3])
    sums = [jnp.sum(total[q]) / total_rows for q in range(4)]
    loss_out[0] = LN2 * sums[0] + (sums[2] - sums[1])
    temp_out[0] = scal[0] * sums[3]
    bias_out[0] = sums[2]
    for k in range(SEG):
        put(k, False).wait()
        put(k, True).wait()
    for k in range(SEG):
        img(k).wait_send()
        own(k).wait_send()
        col(k).wait_send()
        fwd(k).wait_send()
        q_send(k).wait_send()
        for copy in (u_send(k), v_send(k), b_send(k)):
            copy.wait_send()
    u_send(early).wait_recv()
    v_send(early).wait_recv()


def finish(first_late, scal, img, txt, u_own, u_in, v_own, v_in, img_out, txt_out):
    def project(emb, total, out):
        emb32 = emb[...].astype(F32)
        inv_norm = lax.rsqrt(jnp.sum(emb32 * emb32, axis=-1, keepdims=True))
        unit_rows = emb32 * inv_norm
        grad_dir = (total * scal[0]).T
        radial = jnp.sum(unit_rows * grad_dir, axis=-1, keepdims=True)
        out[...] = (grad_dir - unit_rows * radial) * inv_norm

    late = pl.program_id(0) >= first_late

    @pl.when(late)
    def _():
        project(img, u_own[...] + u_in[...], img_out)
        project(txt, v_own[...] + v_in[...], txt_out)

    @pl.when(jnp.logical_not(late))
    def _():
        project(img, u_own[...], img_out)
        project(txt, v_own[...], txt_out)


def solution(mesh):
    group_size = mesh.shape['dp']

    def local_fn(img_emb, txt_emb, log_temp, logit_bias):
        rows, dim = img_emb.shape
        total_rows = rows * group_size
        scal = jnp.stack([jnp.exp(log_temp), logit_bias])
        nblk, kblk = rows // LANE, dim // LANE
        half_out = jax.ShapeDtypeStruct((dim, rows), F32)
        any_spec = pl.BlockSpec(memory_space=pl.ANY)
        smem_spec = pl.BlockSpec(memory_space=pltpu.SMEM)
        dma = pltpu.SemaphoreType.DMA
        u_own, v_own, u_in, v_in, _, loss, grad_temp, grad_bias = pl.pallas_call(
            functools.partial(kernel, float(total_rows)),
            out_shape=[half_out] * 5 + [jax.ShapeDtypeStruct((1,), F32)] * 3,
            in_specs=[smem_spec] + [any_spec] * 2,
            out_specs=[any_spec] * 5 + [smem_spec] * 3,
            scratch_shapes=[
                pltpu.VMEM((4, 8, HC), F32),
                pltpu.VMEM((2, 4, 8, LANE), F32),
                pltpu.VMEM((4, 4, 8, LANE), F32),
                pltpu.VMEM((kblk, 2 * rows, LANE), BF16),
                pltpu.VMEM((2 * nblk, dim, LANE), BF16),
                pltpu.VMEM((4 * nblk, dim, LANE), BF16),
                pltpu.VMEM((dim, 2 * rows), F32),
                pltpu.VMEM((dim, 4 * rows), F32),
                pltpu.VMEM((TR, TC), F32),
                pltpu.VMEM((TR, TC), F32),
                pltpu.VMEM((TC // LANE, TR, LANE), BF16),
                pltpu.VMEM((TC // LANE, TR, LANE), BF16),
                pltpu.VMEM((2, dim, HALF), F32),
                dma((kblk,)),
                dma((SEG * kblk,)),
            ] + [dma((SEG,))] * 16 + [dma((2 * SEG,)), dma((4,)), dma((4,)), dma((2,)), pltpu.SemaphoreType.REGULAR],
            compiler_params=pltpu.CompilerParams(
                collective_id=0, has_side_effects=True, vmem_limit_bytes=67043328),
        )(scal, img_emb, txt_emb)
        step_rows = 256
        first_late = (SEG - 1) * TR // step_rows
        emb_spec = pl.BlockSpec((step_rows, dim), lambda i: (i, 0))
        col_spec = pl.BlockSpec((dim, step_rows), lambda i: (0, i))
        late_spec = pl.BlockSpec((dim, step_rows), lambda i: (0, jnp.maximum(i, first_late)))
        grad_img, grad_txt = pl.pallas_call(
            functools.partial(finish, first_late),
            grid=(rows // step_rows,),
            out_shape=[jax.ShapeDtypeStruct((rows, dim), F32)] * 2,
            in_specs=[smem_spec] + [emb_spec] * 2 + [col_spec, late_spec] * 2,
            out_specs=[emb_spec] * 2,
        )(scal, img_emb, txt_emb, u_own, u_in, v_own, v_in)
        return loss[0], grad_img, grad_txt, grad_temp[0], grad_bias[0]

    return jax.shard_map(
        local_fn,
        mesh=mesh,
        in_specs=(P('dp', None), P('dp', None), P(), P()),
        out_specs=(P(), P('dp', None), P('dp', None), P(), P()),
        check_vma=False,
    )
```
